128 devices in a mesh: seq: 64 (over y, z, x), head: 2 (over core).
Axes of the slice: x: 4, y: 4, z: 4, core: 2. Of those that a mesh axis runs over, the one named last changes fastest.
Arguments:
- query: bfloat16 [8192, 8, 256], P('seq', 'head'), may hold values from -0.6 to 0.6
- key: bfloat16 [8192, 8, 256], P('seq', 'head'), may hold values from -0.59765625 to 0.59765625
- value: bfloat16 [8192, 8, 512], P('seq', 'head'), may hold values from -0.59765625 to 0.59765625
- out_grad: bfloat16 [8192, 8, 512], P(('seq', 'head')), may hold values from -0.6 to 0.6
- log_decay: bfloat16 [8192, 8, 256], P('seq', 'head'), may hold values from -0.1 to 0, as said below
- checkpoints: bfloat16 [64, 8, 256, 512], P('seq', 'head'), may hold values from -12 to 12
Outputs:
- grad_query: bfloat16 [8192, 8, 256], P('seq', 'head')
- grad_key: bfloat16 [8192, 8, 256], P('seq', 'head')
- grad_value: bfloat16 [8192, 8, 512], P('seq', 'head')
- grad_decay: bfloat16 [8192, 8, 256], P('seq', 'head')
The draws below stay inside these ranges and needn't reach their ends.
Inputs may be any that keep to these rules, and one draw needn't show every extreme that they name: `log_decay`: every entry is negative.
All inputs are finite; a program needn't handle non-finite values.
Results may differ from the reference program's by a relative error of at most 0.001.
Values may be sent and summed in bfloat16 or wider, within the bound.
No kernel may reach another device: no remote copies, remote signals or barrier semaphores. Data moves between devices by JAX's collectives and lax.ppermute only.
A program may use at most 384 MiB of HBM per device.

```python
import math
import jax
import jax.numpy as jnp
from jax import lax

HEADS = 8
DK = 256
DV = 512
BLOCK = 64
TOK_DEV = 128
LENGTH = 8192
SEGMENTS = 64


def draw_log_decay(key, part):
    keys = jax.random.split(key, 5)
    share = 0.5
    forgets = jax.random.uniform(keys[0], (HEADS, DK), jnp.float32) < share
    fast = jnp.exp(jax.random.uniform(keys[1], (HEADS, DK), jnp.float32, math.log(1.0 / 400.0), math.log(1.0 / 30.0)))
    slow = jnp.exp(jax.random.uniform(keys[2], (HEADS, DK), jnp.float32, math.log(0.1), math.log(1.5))) / LENGTH
    base = jnp.where(forgets, fast, slow)
    rough = jax.random.uniform(keys[3], (LENGTH, HEADS, DK), jnp.float32, 0.5, 1.5)
    segment = jnp.exp(jax.random.uniform(keys[4], (LENGTH // TOK_DEV, HEADS, DK), jnp.float32, math.log(0.005), math.log(2.0)))
    factor = jnp.repeat(segment, TOK_DEV, axis=0)
    rate = jnp.minimum(base[None] * rough * factor, 0.1)
    return (-rate).astype(jnp.bfloat16)


def draw_query(key, part):
    keys = jax.random.split(jax.random.fold_in(key, 11), 1)
    values = 0.1 * jax.random.normal(keys[0], (LENGTH, HEADS, DK), jnp.float32)
    return jnp.clip(values, -0.6, 0.6).astype(jnp.bfloat16)


def draw_out_grad(key, part):
    keys = jax.random.split(jax.random.fold_in(key, 23), 3)
    segment = jnp.exp(jax.random.uniform(keys[2], (LENGTH // TOK_DEV, 1, 1), jnp.float32, -3.5, 0.0))
    level = jnp.repeat(segment, TOK_DEV, axis=0)
    values = level * 0.1 * jax.random.normal(keys[0], (LENGTH, HEADS, DV), jnp.float32)
    return jnp.clip(values, -0.6, 0.6).astype(jnp.bfloat16)


def levels(stream_key, dims, shards, low, largest):
    factor_of = 1.0
    for axis_at, parts in shards:
        draws = jax.random.uniform(jax.random.fold_in(jax.random.fold_in(stream_key, 6), axis_at), (parts,), jnp.float32, low / len(shards), largest / len(shards))
        factor_of = factor_of * jnp.repeat(jnp.exp(draws), dims[axis_at] // parts).reshape((-1,) + (1,) * (len(dims) - 1 - axis_at))
    return factor_of


def bell_draw(stream_key, shape, width, bound, cuts=(), held_as=jnp.bfloat16):
    drawn = jax.random.normal(stream_key, shape, jnp.float32) * width
    if len(cuts) > 0:
        drawn = levels(stream_key, shape, cuts, -0.22, 0.18) * drawn
    return jnp.clip(drawn, min=-bound, max=bound).astype(held_as)


def setup_inputs(seed: int = 0) -> dict:
    arg_keys = jax.random.split(jax.random.key(seed), 7)
    return {
        "query": draw_query(jax.random.fold_in(arg_keys[6], 71), 0),
        "key": bell_draw(arg_keys[1], (LENGTH, HEADS, DK), 0.1, 0.59765625, ((0, 64), (1, 2))),
        "value": bell_draw(arg_keys[2], (LENGTH, HEADS, DV), 0.1, 0.59765625, ((0, 64), (1, 2))),
        "out_grad": draw_out_grad(jax.random.fold_in(arg_keys[6], 71), 0),
        "log_decay": draw_log_decay(jax.random.fold_in(arg_keys[6], 71), 0),
        "checkpoints": bell_draw(arg_keys[5], (SEGMENTS, HEADS, DK, DV), 2.0, 12.0, ((0, 64), (1, 2))),
    }


PRECISE = lax.Precision.HIGHEST


def reference(query, key, value, out_grad, log_decay, checkpoints):
    length, head_count, width_key = query.shape
    width_value = value.shape[-1]
    scaling = width_key ** -0.5
    blocks = length // BLOCK
    segment_count = length // TOK_DEV
    per_segment = TOK_DEV // BLOCK

    def blocked(array):
        return array.reshape(blocks, BLOCK, head_count, array.shape[-1])

    row_index = lax.broadcasted_iota(jnp.int32, (BLOCK, BLOCK), 0)
    col_index = lax.broadcasted_iota(jnp.int32, (BLOCK, BLOCK), 1)
    causal = (col_index <= row_index).astype(jnp.float32)

    def forward(carried, inputs):
        query_block, key_block, value_block, grad_block, decay_block = tuple(member.astype(jnp.float32) for member in inputs)
        inside = jnp.cumsum(decay_block, axis=0)
        block_end = inside[-1]
        key_fall = key_block * jnp.exp(-inside)
        scores = jnp.einsum("thj,uhj->htu", grad_block, value_block, precision=PRECISE) * causal
        near = jnp.einsum("htu,uhc->thc", scores, key_fall, precision=PRECISE)
        reached = jnp.einsum("thj,hcj->thc", grad_block, carried, precision=PRECISE)
        query_grad = scaling * jnp.exp(inside) * (reached + near)
        key_end = key_block * jnp.exp(block_end - inside)
        carried = jnp.exp(block_end)[..., None] * carried + jnp.einsum("thc,thj->hcj", key_end, value_block, precision=PRECISE)
        return carried, query_grad

    def backward(carried, inputs):
        query_block, key_block, value_block, grad_block, decay_block = tuple(member.astype(jnp.float32) for member in inputs)
        inside = jnp.cumsum(decay_block, axis=0)
        block_end = inside[-1]
        query_rise = query_block * jnp.exp(inside)
        key_fall = key_block * jnp.exp(-inside)
        to_end = jnp.exp(block_end - inside)
        scores = jnp.einsum("thj,uhj->htu", grad_block, value_block, precision=PRECISE) * causal
        affinity = jnp.einsum("thc,uhc->htu", query_rise, key_fall, precision=PRECISE) * causal
        key_grad = scaling * jnp.exp(-inside) * jnp.einsum("htu,thc->uhc", scores, query_rise, precision=PRECISE)
        key_grad = key_grad + to_end * jnp.einsum("thj,hcj->thc", value_block, carried, precision=PRECISE)
        value_grad = scaling * jnp.einsum("htu,thj->uhj", affinity, grad_block, precision=PRECISE)
        value_grad = value_grad + jnp.einsum("thc,hcj->thj", key_block * to_end, carried, precision=PRECISE)
        carried = jnp.exp(block_end)[..., None] * carried + scaling * jnp.einsum("thc,thj->hcj", query_rise, grad_block, precision=PRECISE)
        return carried, (key_grad, value_grad)

    sliced = (blocked(query), blocked(key), blocked(value), blocked(out_grad), blocked(log_decay))

    def by_segment(array):
        return array.reshape((segment_count, per_segment) + array.shape[1:])

    segmented = tuple(by_segment(member) for member in sliced)

    def segment_forward(pair):
        start, inputs = pair
        unused, produced = lax.scan(forward, start.astype(jnp.float32), inputs)
        return produced

    query_grad = lax.map(segment_forward, (checkpoints, segmented))
    empty_state = jnp.zeros((head_count, width_key, width_value), jnp.float32)
    unused_grad, (key_grad, value_grad) = lax.scan(backward, empty_state, sliced, reverse=True)
    query_flat = query_grad.reshape(length, head_count, width_key)
    key_flat = key_grad.reshape(length, head_count, width_key)
    value_flat = value_grad.reshape(length, head_count, width_value)
    weight = query.astype(jnp.float32) * query_flat - key.astype(jnp.float32) * key_flat
    decay_grad = lax.cumsum(weight, axis=0, reverse=True)
    return (query_flat.astype(jnp.bfloat16), key_flat.astype(jnp.bfloat16),
            value_flat.astype(jnp.bfloat16), decay_grad.astype(jnp.bfloat16))
```

```python
import jax
import jax.numpy as jnp
from jax import lax
from jax.experimental import pallas as pl
from jax.experimental.pallas import tpu as pltpu
from jax.sharding import Mesh
from jax.sharding import PartitionSpec as P


Y, Z, X, H = "seq_0", "seq_1", "seq_2", "head"
SEQ = (Y, Z, X)
F32 = jnp.float32
B16 = jnp.bfloat16
NN = ((1,), (0,))
NT = ((1,), (1,))
TN = ((0,), (0,))
TOK, NH, DK, DV = 128, 4, 256, 512
SCALE = DK ** (-0.5)


def split(x):
    high = x.astype(B16)
    return high, (x - high.astype(F32)).astype(B16)


def dot(a, b, dims):
    return lax.dot_general(a, b, (dims, ((), ())), preferred_element_type=F32)


def dot2(a, b, dims):
    high, low = split(a)
    return dot(high, b, dims) + dot(low, b, dims)


def dot3(a, b, dims):
    a_high, a_low = split(a)
    b_high, b_low = split(b)
    return dot(a_high, b_high, dims) + (dot(a_low, b_high, dims) + dot(a_high, b_low, dims))


def triangle(upper):
    row = lax.broadcasted_iota(jnp.int32, (TOK, TOK), 0)
    col = lax.broadcasted_iota(jnp.int32, (TOK, TOK), 1)
    return (col >= row) if upper else (col <= row)


def sds(shape, dtype=B16):
    return jax.ShapeDtypeStruct(shape, dtype)


def call(body, outs, n_in, scratch=(), name=None):
    specs = [pl.BlockSpec(memory_space=pltpu.SMEM)]
    specs += [pl.BlockSpec(memory_space=pltpu.VMEM)] * n_in
    return pl.pallas_call(
        body, out_shape=outs, in_specs=specs, scratch_shapes=list(scratch), name=name
    )


def pack_grad(idx, g, send, keep, scr):
    for h in range(2 * NH):
        scr[h] = g[:, h, :]
    c = idx[3]
    for i in range(NH):
        send[i] = scr[NH * (1 - c) + i]
        keep[i] = scr[NH * c + i]


def pack_pair(idx, a, b, *rest):
    outs, scr = rest[:4], rest[4]
    width = a.shape[-1]
    for h in range(NH):
        scr[h, :, :width] = a[:, h, :]
        scr[h, :, width:] = b[:, h, :]
    for s in range(4):
        outs[s][...] = scr[(idx[0] + s) % 4]


def join_grad(idx, keep, recv, *outs):
    c = idx[3]
    half = TOK // 2
    for s in range(4):
        h = (idx[0] + s) % 4
        outs[s][pl.ds(pl.multiple_of(half * c, half), half), :] = keep[h]
        outs[s][pl.ds(pl.multiple_of(half * (1 - c), half), half), :] = recv[h]


def query_part(idx, *refs):
    qa, gr, kv = refs[0:4], refs[4:8], refs[8:12]
    check = refs[12]
    dq_out, qdq_out = refs[13:15]
    kv_out = refs[15:19]
    scr = refs[19]
    low = triangle(False)
    tri = low.astype(B16)
    for s in range(4):
        h = (idx[0] + s) % 4
        q = qa[s][:, :DK].astype(F32)
        cum = dot(tri, qa[s][:, DK:], NN)
        k = kv[s][:, :DK].astype(F32)
        g = gr[s][...]
        scores = jnp.where(low, dot(g, kv[s][:, DK:], NT), 0.0)
        reached = dot(g, check[0, h], NT) + dot3(scores, k * jnp.exp(-cum), NN)
        dq = SCALE * jnp.exp(cum) * reached
        scr[h] = dq
        qdq = q * dq
        qdq_out[h] = qdq
        total = jnp.sum(qdq, axis=0, keepdims=True)
        t0 = total.astype(B16)
        rest = total - t0.astype(F32)
        t1 = rest.astype(B16)
        t2 = (rest - t1.astype(F32)).astype(B16)
        kv_out[s][:TOK, :] = kv[s][...]
        kv_out[s][TOK:, :DK] = jnp.broadcast_to(t0, (16, DK))
        kv_out[s][TOK:, DK : 2 * DK] = jnp.broadcast_to(t1, (16, DK))
        kv_out[s][TOK:, 2 * DK :] = jnp.broadcast_to(t2, (16, DK))
    for h in range(NH):
        dq_out[:, h, :] = scr[h].astype(B16)


def line_state(idx, *refs):
    qa, gr = refs[0:4], refs[4:8]
    chunks = refs[8:12]
    cum_out, qa_out, g_out = refs[12:15]
    acc = refs[15]
    x, z = idx[0], idx[1]
    for s in range(4):
        j = (x - s + 4) % 4
        rows = pl.ds(pl.multiple_of(TOK * j, TOK), TOK)
        qa_out[rows, :] = qa[s][...]
        g_out[rows, :] = gr[s][...]
    tri = triangle(False).astype(B16)
    base = jnp.zeros((1, DK), F32)
    for j in range(4):
        rows = slice(TOK * j, TOK * (j + 1))
        cum = dot(tri, qa_out[rows, DK:], NN) + base
        base = cum[TOK - 1 :, :]
        cum_out[rows, :] = cum
    rise = qa_out[:, :DK].astype(F32) * jnp.exp(cum_out[...])
    high, lo = split(SCALE * rise)
    g = g_out[...]
    acc[...] = dot(g, high, TN) + dot(g, lo, TN)
    for s in range(4):
        at = pl.multiple_of(TOK * ((z + s) % 4), TOK)
        chunks[s][:TOK, :] = acc[pl.ds(at, TOK), :]
        chunks[s][TOK:, :] = jnp.broadcast_to(base, (8, DK))


def scan_z(idx, *refs):
    parts = refs[0:4]
    total, suffix = refs[4:6]
    scr = refs[6]
    z = idx[1]
    for s in range(4):
        scr[(z - s + 4) % 4] = parts[s][...]
    state = jnp.zeros((TOK, DK), F32)
    logs = jnp.zeros((1, DK), F32)
    for j in reversed(range(4)):
        suffix[j, :TOK, :] = state
        suffix[j, TOK:, :] = jnp.broadcast_to(logs, (8, DK))
        own = scr[j, TOK : TOK + 1, :]
        state = jnp.exp(own) * state + scr[j, :TOK, :]
        logs = logs + own
    total[:TOK, :] = state
    total[TOK:, :] = jnp.broadcast_to(logs, (8, DK))


def scan_y(idx, *refs):
    parts, suffix = refs[0:4], refs[4]
    outs = refs[5:9]
    scr = refs[9]
    y, z = idx[2], idx[1]
    for s in range(4):
        scr[(y - s + 4) % 4] = parts[s][...]
    state = jnp.zeros((TOK, DK), F32)
    for j in (3, 2, 1):
        joined = jnp.exp(scr[j, TOK : TOK + 1, :]) * state + scr[j, :TOK, :]
        state = jnp.where(j > y, joined, state)
    for s in range(4):
        j = (z + s) % 4
        outs[s][...] = suffix[j, :TOK, :] + jnp.exp(suffix[j, TOK : TOK + 1, :]) * state


def near_part(idx, *refs):
    qa, g, cum = refs[0:3]
    kv = refs[3:7]
    dk_near, dv_near, k_end, ends, v_out, k_out = refs[7:13]
    rise = refs[13]
    x = idx[0]
    for s in range(4):
        j = (x - s + 4) % 4
        rows = pl.ds(pl.multiple_of(TOK * j, TOK), TOK)
        k_out[rows, :] = kv[s][:TOK, :DK]
        v_out[rows, :] = kv[s][:TOK, DK:]
    rise[...] = SCALE * qa[:, :DK].astype(F32) * jnp.exp(cum[...])
    last = cum[4 * TOK - 1 :, :]
    end = jnp.exp(last - cum[...])
    ends[...] = end
    k_end[...] = k_out[...].astype(F32) * end
    upper = triangle(True)
    for j in range(4):
        rows = slice(TOK * j, TOK * (j + 1))
        width = 4 * TOK - TOK * j
        later = slice(TOK * j, 4 * TOK)
        fall = jnp.exp(-cum[rows, :])
        keep = lax.broadcasted_iota(jnp.int32, (TOK, width), 1) >= lax.broadcasted_iota(
            jnp.int32, (TOK, width), 0
        )
        scores = jnp.where(keep, dot(v_out[rows, :], g[later, :], NT), 0.0)
        dk_near[rows, :] = fall * dot3(scores, rise[later, :], NN)
        k_fall = k_out[rows, :].astype(F32) * fall
        affinity = jnp.where(keep, dot3(k_fall, rise[later, :], NT), 0.0)
        dv_near[rows, :] = dot2(affinity, g[later, :], NN)


def far_part(idx, *refs):
    parts = refs[0:4]
    kv = refs[4:8]
    dk_near, dv_near, k_end, ends, v, k = refs[8:14]
    outs = refs[14:18]
    sums = refs[18]
    state, scr = refs[19:21]
    x, z = idx[0], idx[1]
    for s in range(4):
        j = (z - s + 4) % 4
        state[pl.ds(pl.multiple_of(TOK * j, TOK), TOK), :] = parts[s][...]
    high, lo = split(state[...])
    reached = dot(v[...], high, NN) + dot(v[...], lo, NN)
    dk = dk_near[...] + ends[...] * reached
    dk_high, dk_low = split(dk)
    e_high, e_low = split(k_end[...])
    dv = dv_near[...] + (
        dot(e_high, high, NT) + (dot(e_low, high, NT) + dot(e_high, lo, NT))
    )
    kdk = k[...].astype(F32) * dk
    for j in range(4):
        rows = slice(TOK * j, TOK * (j + 1))
        scr[j, :, :DK] = dk_high[rows, :]
        scr[j, :, DK : 2 * DK] = dk_low[rows, :]
        scr[j, :, 2 * DK :] = dv[rows, :].astype(B16)
        sums[j : j + 1, :] = -jnp.sum(kdk[rows, :], axis=0, keepdims=True)
    for s in range(4):
        j = (x - s + 4) % 4
        tot = (
            kv[s][TOK : TOK + 1, :DK].astype(F32)
            + kv[s][TOK : TOK + 1, DK : 2 * DK].astype(F32)
            + kv[s][TOK : TOK + 1, 2 * DK :].astype(F32)
        )
        sums[pl.ds(j, 1), :] = sums[pl.ds(j, 1), :] + tot
    sums[4:5, :] = jnp.sum(sums[0:4, :], axis=0, keepdims=True)
    sums[5:8, :] = jnp.zeros((3, DK), F32)
    for s in range(4):
        outs[s][...] = scr[(x + s) % 4]


def final_part(idx, *refs):
    parts, later = refs[0:4], refs[4:8]
    qdq = refs[8]
    kv = refs[9:13]
    dk_out, dv_out, da_out = refs[13:16]
    s_dk, s_dv, s_da, s_k = refs[16:20]
    x = idx[0]
    for s in range(4):
        s_k[(x + s) % 4] = kv[s][:TOK, :DK]
    upper = triangle(True).astype(B16)
    for s in range(4):
        h = (x - s + 4) % 4
        dk_high = parts[s][:, :DK]
        dk = dk_high.astype(F32) + parts[s][:, DK : 2 * DK].astype(F32)
        s_dk[h] = dk_high
        s_dv[h] = parts[s][:, 2 * DK :]
        weight = qdq[h] - s_k[h].astype(F32) * dk
        w_high, w_low = split(weight)
        da = dot(upper, w_high, NN) + dot(upper, w_low, NN) + later[s][pl.ds(x, 1), :]
        s_da[h] = da.astype(B16)
    for h in range(NH):
        dk_out[:, h, :] = s_dk[h]
        dv_out[:, h, :] = s_dv[h]
        da_out[:, h, :] = s_da[h]


def shifted(value, axis, s):
    return lax.ppermute(value, axis, [(i, (i + s) % 4) for i in range(4)])


def spread(parts, axis):
    return [parts[0]] + [shifted(parts[s], axis, s) for s in (1, 2, 3)]


def per_device(query, key, value, out_grad, log_decay, checkpoints):
    x, z, y, c = (lax.axis_index(axis) for axis in (X, Z, Y, H))
    idx = jnp.stack([x, z, y, c]).astype(jnp.int32)
    vm = pltpu.VMEM

    half = TOK // 2
    send, keep = call(
        pack_grad,
        [sds((NH, half, DV))] * 2,
        1,
        [vm((2 * NH, half, DV), B16)],
        "pack_grad",
    )(idx, out_grad)
    recv = lax.ppermute(send, H, [(0, 1), (1, 0)])
    qa = call(
        pack_pair, [sds((TOK, 2 * DK))] * 4, 2, [vm((NH, TOK, 2 * DK), B16)], "pack_qa"
    )(idx, query, log_decay)
    qa_line = spread(qa, X)
    g = call(join_grad, [sds((TOK, DV))] * 4, 2, (), "join_grad")(idx, keep, recv)
    g_line = spread(g, X)
    kv = call(
        pack_pair, [sds((TOK, DK + DV))] * 4, 2, [vm((NH, TOK, DK + DV), B16)], "pack_kv"
    )(idx, key, value)
    res = call(
        query_part,
        [sds((TOK, NH, DK)), sds((NH, TOK, DK), F32)] + [sds((TOK + 16, DK + DV))] * 4,
        13,
        [vm((NH, TOK, DK), F32)],
        "query_part",
    )(idx, *qa, *g, *kv, checkpoints)
    dq, qdq, kv = res[0], res[1], res[2:]
    res = call(
        line_state,
        [sds((TOK + 8, DK), F32)] * 4
        + [sds((4 * TOK, DK), F32), sds((4 * TOK, 2 * DK)), sds((4 * TOK, DV))],
        8,
        [vm((DV, DK), F32)],
        "line_state",
    )(idx, *qa_line, *g_line)
    chunks, cum, qa_rows, g_rows = res[:4], res[4], res[5], res[6]
    z_in = spread(chunks, Z)
    kv_line = spread(kv, X)
    total, suffix = call(
        scan_z,
        [sds((TOK + 8, DK), F32), sds((4, TOK + 8, DK), F32)],
        4,
        [vm((4, TOK + 8, DK), F32)],
        "scan_z",
    )(idx, *z_in)
    y_in = spread([total] * 4, Y)
    carry = call(
        scan_y, [sds((TOK, DK), F32)] * 4, 5, [vm((4, TOK + 8, DK), F32)], "scan_y"
    )(idx, *y_in, suffix)
    carry_in = spread(carry, Z)
    near = call(
        near_part,
        [
            sds((4 * TOK, DK), F32),
            sds((4 * TOK, DV), F32),
            sds((4 * TOK, DK), F32),
            sds((4 * TOK, DK), F32),
            sds((4 * TOK, DV)),
            sds((4 * TOK, DK)),
        ],
        7,
        [vm((4 * TOK, DK), F32)],
        "near_part",
    )(idx, qa_rows, g_rows, cum, *kv_line)
    res = call(
        far_part,
        [sds((TOK, 2 * DK + DV))] * 4 + [sds((8, DK), F32)],
        14,
        [vm((DV, DK), F32), vm((4, TOK, 2 * DK + DV), B16)],
        "far_part",
    )(idx, *carry_in, *kv_line, *near)
    back, sums = res[:4], res[4]
    back_in = spread(back, X)

    def beyond(total, axis, index):
        parts = spread([total] * 4, axis)
        later = jnp.zeros_like(total)
        everything = total
        for s in (1, 2, 3):
            later = later + jnp.where((index - s) % 4 > index, parts[s], 0.0)
            everything = everything + parts[s]
        return later, everything

    line_total = sums[4:5]
    z_later, z_all = beyond(jnp.broadcast_to(line_total, (8, DK)), Z, z)
    y_later, _ = beyond(z_all, Y, y)
    outside = z_later + y_later
    inside = jnp.stack([jnp.sum(sums[j + 1 : 4], axis=0) for j in range(4)])
    later = outside + jnp.concatenate([inside, jnp.zeros((4, DK), F32)])
    later_in = spread([later] * 4, X)
    dk, dv, da = call(
        final_part,
        [sds((TOK, NH, DK)), sds((TOK, NH, DV)), sds((TOK, NH, DK))],
        13,
        [
            vm((NH, TOK, DK), B16),
            vm((NH, TOK, DV), B16),
            vm((NH, TOK, DK), B16),
            vm((NH, TOK, DK), B16),
        ],
        "final_part",
    )(idx, *back_in, *later_in, qdq, *kv)
    return dq, dk, dv, da


def solution(mesh):
    torus = Mesh(mesh.devices.reshape(4, 4, 4, 2), (Y, Z, X, H))
    by_token = P(SEQ, H, None)
    placed = (
        by_token,
        by_token,
        by_token,
        P(SEQ + (H,), None, None),
        by_token,
        P(SEQ, H, None, None),
    )
    return jax.shard_map(
        per_device, mesh=torus, in_specs=placed, out_specs=(by_token,) * 4, check_vma=False
    )
```

```python
import jax
import jax.numpy as jnp
from jax import lax
from jax.experimental import pallas as pl
from jax.experimental.pallas import tpu as pltpu
from jax.sharding import Mesh
from jax.sharding import PartitionSpec as P


Y, Z, X, H = "seq_0", "seq_1", "seq_2", "head"
SEQ = (Y, Z, X)
F32 = jnp.float32
B16 = jnp.bfloat16
NN = ((1,), (0,))
NT = ((1,), (1,))
TN = ((0,), (0,))
TOK, NH, DK, DV = 128, 4, 256, 512
SCALE = DK ** (-0.5)


def split(x):
    high = x.astype(B16)
    return high, (x - high.astype(F32)).astype(B16)


def dot(a, b, dims):
    return lax.dot_general(a, b, (dims, ((), ())), preferred_element_type=F32)


def dot2(a, b, dims):
    high, low = split(a)
    return dot(high, b, dims) + dot(low, b, dims)


def dot3(a, b, dims):
    a_high, a_low = split(a)
    b_high, b_low = split(b)
    return dot(a_high, b_high, dims) + (dot(a_low, b_high, dims) + dot(a_high, b_low, dims))


def triangle(upper):
    row = lax.broadcasted_iota(jnp.int32, (TOK, TOK), 0)
    col = lax.broadcasted_iota(jnp.int32, (TOK, TOK), 1)
    return (col >= row) if upper else (col <= row)


def sds(shape, dtype=B16):
    return jax.ShapeDtypeStruct(shape, dtype)


def call(body, outs, n_in, scratch=(), after=()):
    specs = [pl.BlockSpec(memory_space=pltpu.SMEM)]
    specs += [pl.BlockSpec(memory_space=pltpu.VMEM)] * n_in
    specs += [pl.BlockSpec(memory_space=pl.ANY)] * len(after)

    def ordered(*refs):
        return body(*refs[: 1 + n_in], *refs[1 + n_in + len(after) :])

    run = pl.pallas_call(
        ordered,
        out_shape=outs,
        in_specs=specs,
        scratch_shapes=list(scratch),
        compiler_params=pltpu.CompilerParams(vmem_limit_bytes=16 * 1024 * 1024),
    )
    return lambda *operands: run(*operands, *after)


def pack_grad(idx, g, send, keep, scr):
    for h in range(2 * NH):
        scr[h] = g[:, h, :]
    c = idx[3]
    for i in range(NH):
        send[i] = scr[NH * (1 - c) + i]
        keep[i] = scr[NH * c + i]


def pack_rows(idx, a, b, out):
    width = a.shape[-1]
    for h in range(NH):
        out[h, :, :width] = a[:, h, :]
        out[h, :, width:] = b[:, h, :]


def pack_pair(idx, a, b, *rest):
    outs, scr = rest[:4], rest[4]
    pack_rows(idx, a, b, scr)
    for s in range(4):
        outs[s][...] = scr[(idx[0] + s) % 4]


def join_all(idx, qa, keep, recv, *outs):
    c = idx[3]
    half = TOK // 2
    mine = pl.ds(pl.multiple_of(half * c, half), half)
    theirs = pl.ds(pl.multiple_of(half * (1 - c), half), half)
    for s in range(4):
        h = (idx[0] + s) % 4
        outs[s][:, : 2 * DK] = qa[h]
        outs[s][mine, 2 * DK :] = keep[h]
        outs[s][theirs, 2 * DK :] = recv[h]


def query_part(idx, *refs):
    qag, kv = refs[0:4], refs[4:8]
    check = refs[8]
    dq_out, qdq_out = refs[9:11]
    kv_out = refs[11:15]
    scr = refs[15]
    low = triangle(False)
    tri = low.astype(B16)
    for s in range(4):
        h = (idx[0] + s) % 4
        q = qag[s][:, :DK].astype(F32)
        cum = dot(tri, qag[s][:, DK : 2 * DK], NN)
        k = kv[s][:, :DK].astype(F32)
        g = qag[s][:, 2 * DK :]
        scores = jnp.where(low, dot(g, kv[s][:, DK:], NT), 0.0)
        reached = dot(g, check[0, h], NT) + dot3(scores, k * jnp.exp(-cum), NN)
        dq = SCALE * jnp.exp(cum) * reached
        scr[h] = dq
        qdq = q * dq
        qdq_out[h] = qdq
        total = jnp.sum(qdq, axis=0, keepdims=True)
        t0 = total.astype(B16)
        rest = total - t0.astype(F32)
        t1 = rest.astype(B16)
        t2 = (rest - t1.astype(F32)).astype(B16)
        kv_out[s][:TOK, :] = kv[s][...]
        kv_out[s][TOK:, :DK] = jnp.broadcast_to(t0, (16, DK))
        kv_out[s][TOK:, DK : 2 * DK] = jnp.broadcast_to(t1, (16, DK))
        kv_out[s][TOK:, 2 * DK :] = jnp.broadcast_to(t2, (16, DK))
    for h in range(NH):
        dq_out[:, h, :] = scr[h].astype(B16)


def line_cum(qa, cum_scr):
    tri = triangle(False).astype(B16)
    base = jnp.zeros((1, DK), F32)
    for j in range(4):
        rows = slice(TOK * j, TOK * (j + 1))
        cum = dot(tri, qa[rows, DK:], NN) + base
        base = cum[TOK - 1 :, :]
        cum_scr[rows, :] = cum
    return base


def line_state(idx, *refs):
    qag = refs[0:4]
    chunks = refs[4:8]
    qa_out, g_out = refs[8:10]
    acc, cum_scr = refs[10:12]
    x, z = idx[0], idx[1]
    for s in range(4):
        j = (x - s + 4) % 4
        rows = pl.ds(pl.multiple_of(TOK * j, TOK), TOK)
        qa_out[rows, :] = qag[s][:, : 2 * DK]
        g_out[rows, :] = qag[s][:, 2 * DK :]
    base = line_cum(qa_out, cum_scr)
    rise = qa_out[:, :DK].astype(F32) * jnp.exp(cum_scr[...])
    high, lo = split(SCALE * rise)
    g = g_out[...]
    acc[...] = dot(g, high, TN) + dot(g, lo, TN)
    for s in range(4):
        at = pl.multiple_of(TOK * ((z + s) % 4), TOK)
        chunks[s][:TOK, :] = acc[pl.ds(at, TOK), :]
        chunks[s][TOK:, :] = jnp.broadcast_to(base, (8, DK))


def scan_z(idx, *refs):
    parts = refs[0:4]
    total, suffix = refs[4:6]
    scr = refs[6]
    z = idx[1]
    for s in range(4):
        scr[(z - s + 4) % 4] = parts[s][...]
    state = jnp.zeros((TOK, DK), F32)
    logs = jnp.zeros((1, DK), F32)
    for j in reversed(range(4)):
        suffix[j, :TOK, :] = state
        suffix[j, TOK:, :] = jnp.broadcast_to(logs, (8, DK))
        own = scr[j, TOK : TOK + 1, :]
        state = jnp.exp(own) * state + scr[j, :TOK, :]
        logs = logs + own
    total[:TOK, :] = state
    total[TOK:, :] = jnp.broadcast_to(logs, (8, DK))


def scan_y(idx, *refs):
    parts, suffix = refs[0:4], refs[4]
    outs, token = refs[5:9], refs[9]
    scr = refs[10]
    y, z = idx[2], idx[1]
    token[...] = jnp.zeros((8, 128), F32)
    for s in range(4):
        scr[(y - s + 4) % 4] = parts[s][...]
    state = jnp.zeros((TOK, DK), F32)
    for j in (3, 2, 1):
        joined = jnp.exp(scr[j, TOK : TOK + 1, :]) * state + scr[j, :TOK, :]
        state = jnp.where(j > y, joined, state)
    for s in range(4):
        j = (z + s) % 4
        outs[s][...] = suffix[j, :TOK, :] + jnp.exp(suffix[j, TOK : TOK + 1, :]) * state


def near_part(idx, *refs):
    qa, g = refs[0:2]
    kv = refs[2:6]
    dk_near, dv_near, k_end, ends, v_out, k_out = refs[6:12]
    rise, cum = refs[12:14]
    last = line_cum(qa, cum)
    x = idx[0]
    for s in range(4):
        j = (x - s + 4) % 4
        rows = pl.ds(pl.multiple_of(TOK * j, TOK), TOK)
        k_out[rows, :] = kv[s][:TOK, :DK]
        v_out[rows, :] = kv[s][:TOK, DK:]
    rise[...] = SCALE * qa[:, :DK].astype(F32) * jnp.exp(cum[...])
    end = jnp.exp(last - cum[...])
    ends[...] = end
    k_end[...] = k_out[...].astype(F32) * end
    upper = triangle(True)
    for j in range(4):
        rows = slice(TOK * j, TOK * (j + 1))
        width = 4 * TOK - TOK * j
        later = slice(TOK * j, 4 * TOK)
        fall = jnp.exp(-cum[rows, :])
        keep = lax.broadcasted_iota(jnp.int32, (TOK, width), 1) >= lax.broadcasted_iota(
            jnp.int32, (TOK, width), 0
        )
        scores = jnp.where(keep, dot(v_out[rows, :], g[later, :], NT), 0.0)
        dk_near[rows, :] = fall * dot3(scores, rise[later, :], NN)
        k_fall = k_out[rows, :].astype(F32) * fall
        affinity = jnp.where(keep, dot3(k_fall, rise[later, :], NT), 0.0)
        dv_near[rows, :] = dot2(affinity, g[later, :], NN)


def far_part(idx, *refs):
    parts = refs[0:4]
    kv = refs[4:8]
    dk_near, dv_near, k_end, ends, v, k = refs[8:14]
    outs = refs[14:18]
    sums = refs[18]
    state, scr = refs[19:21]
    x, z = idx[0], idx[1]
    for s in range(4):
        j = (z - s + 4) % 4
        state[pl.ds(pl.multiple_of(TOK * j, TOK), TOK), :] = parts[s][...]
    high, lo = split(state[...])
    reached = dot(v[...], high, NN) + dot(v[...], lo, NN)
    dk = dk_near[...] + ends[...] * reached
    dk_high, dk_low = split(dk)
    e_high, e_low = split(k_end[...])
    dv = dv_near[...] + (
        dot(e_high, high, NT) + (dot(e_low, high, NT) + dot(e_high, lo, NT))
    )
    kdk = k[...].astype(F32) * dk
    for j in range(4):
        rows = slice(TOK * j, TOK * (j + 1))
        scr[j, :, :DK] = dk_high[rows, :]
        scr[j, :, DK : 2 * DK] = dk_low[rows, :]
        scr[j, :, 2 * DK :] = dv[rows, :].astype(B16)
        sums[j : j + 1, :] = -jnp.sum(kdk[rows, :], axis=0, keepdims=True)
    for s in range(4):
        j = (x - s + 4) % 4
        tot = (
            kv[s][TOK : TOK + 1, :DK].astype(F32)
            + kv[s][TOK : TOK + 1, DK : 2 * DK].astype(F32)
            + kv[s][TOK : TOK + 1, 2 * DK :].astype(F32)
        )
        sums[pl.ds(j, 1), :] = sums[pl.ds(j, 1), :] + tot
    sums[4:5, :] = jnp.sum(sums[0:4, :], axis=0, keepdims=True)
    sums[5:8, :] = jnp.zeros((3, DK), F32)
    for s in range(4):
        outs[s][...] = scr[(x + s) % 4]


def final_part(idx, *refs):
    parts, later = refs[0:4], refs[4:8]
    qdq = refs[8]
    key = refs[9]
    dk_out, dv_out, da_out = refs[10:13]
    s_dk, s_dv, s_da, s_k = refs[13:17]
    x = idx[0]
    for h in range(NH):
        s_k[h] = key[:, h, :]
    upper = triangle(True).astype(B16)
    for s in range(4):
        h = (x - s + 4) % 4
        dk_high = parts[s][:, :DK]
        dk = dk_high.astype(F32) + parts[s][:, DK : 2 * DK].astype(F32)
        s_dk[h] = dk_high
        s_dv[h] = parts[s][:, 2 * DK :]
        weight = qdq[h] - s_k[h].astype(F32) * dk
        w_high, w_low = split(weight)
        da = dot(upper, w_high, NN) + dot(upper, w_low, NN) + later[s][pl.ds(x, 1), :]
        s_da[h] = da.astype(B16)
    for h in range(NH):
        dk_out[:, h, :] = s_dk[h]
        dv_out[:, h, :] = s_dv[h]
        da_out[:, h, :] = s_da[h]


def shifted(value, axis, s):
    return lax.ppermute(value, axis, [(i, (i + s) % 4) for i in range(4)])


def spread(parts, axis):
    moved = [parts[0]]
    for s in (1, 2, 3):
        moved.append(shifted(parts[s], axis, s))
    return moved


def whole(query, key, value, out_grad, log_decay, checkpoints):
    x, z, y, c = (lax.axis_index(axis) for axis in (X, Z, Y, H))
    idx = jnp.stack([x, z, y, c]).astype(jnp.int32)
    vm = pltpu.VMEM

    half = TOK // 2
    send, keep = call(
        pack_grad, [sds((NH, half, DV))] * 2, 1, [vm((2 * NH, half, DV), B16)]
    )(idx, out_grad)
    recv = lax.ppermute(send, H, [(0, 1), (1, 0)])
    qa = call(pack_rows, sds((NH, TOK, 2 * DK)), 2, ())(idx, query, log_decay)
    qag = call(join_all, [sds((TOK, 2 * DK + DV))] * 4, 3, ())(idx, qa, keep, recv)
    qag_line = spread(qag, X)
    kv = call(
        pack_pair, [sds((TOK, DK + DV))] * 4, 2, [vm((NH, TOK, DK + DV), B16)]
    )(idx, key, value)
    res = call(
        query_part,
        [sds((TOK, NH, DK)), sds((NH, TOK, DK), F32)] + [sds((TOK + 16, DK + DV))] * 4,
        9,
        [vm((NH, TOK, DK), F32)],
    )(idx, *qag, *kv, checkpoints)
    dq, qdq, kv = res[0], res[1], res[2:]
    res = call(
        line_state,
        [sds((TOK + 8, DK), F32)] * 4
        + [sds((4 * TOK, 2 * DK)), sds((4 * TOK, DV))],
        4,
        [vm((DV, DK), F32), vm((4 * TOK, DK), F32)],
        (qdq,),
    )(idx, *qag_line)
    chunks, qa_rows, g_rows = res[:4], res[4], res[5]
    z_in = spread(chunks, Z)
    kv_line = spread(kv, X)
    total, suffix = call(
        scan_z,
        [sds((TOK + 8, DK), F32), sds((4, TOK + 8, DK), F32)],
        4,
        [vm((4, TOK + 8, DK), F32)],
    )(idx, *z_in)
    y_in = spread([total] * 4, Y)
    *carry, token = call(
        scan_y, [sds((TOK, DK), F32)] * 4 + [sds((8, 128), F32)], 5, [vm((4, TOK + 8, DK), F32)]
    )(idx, *y_in, suffix)
    carry_in = spread(carry, Z)
    near = call(
        near_part,
        [
            sds((4 * TOK, DK), F32),
            sds((4 * TOK, DV), F32),
            sds((4 * TOK, DK), F32),
            sds((4 * TOK, DK), F32),
            sds((4 * TOK, DV)),
            sds((4 * TOK, DK)),
        ],
        6,
        [vm((4 * TOK, DK), F32)] * 2,
        (token,),
    )(idx, qa_rows, g_rows, *kv_line)
    res = call(
        far_part,
        [sds((TOK, 2 * DK + DV))] * 4 + [sds((8, DK), F32)],
        14,
        [vm((DV, DK), F32), vm((4, TOK, 2 * DK + DV), B16)],
    )(idx, *carry_in, *kv_line, *near)
    back, sums = res[:4], res[4]
    back_in = spread(back, X)

    def beyond(total, axis, index):
        parts = spread([total] * 4, axis)
        later = jnp.zeros_like(total)
        everything = total
        for s in (1, 2, 3):
            later = later + jnp.where((index - s) % 4 > index, parts[s], 0.0)
            everything = everything + parts[s]
        return later, everything

    line_total = sums[4:5]
    z_later, z_all = beyond(jnp.broadcast_to(line_total, (8, DK)), Z, z)
    y_later, _ = beyond(z_all, Y, y)
    outside = z_later + y_later
    inside = jnp.stack([jnp.sum(sums[j + 1 : 4], axis=0) for j in range(4)])
    later = outside + jnp.concatenate([inside, jnp.zeros((4, DK), F32)])
    later_in = spread([later] * 4, X)
    dk, dv, da = call(
        final_part,
        [sds((TOK, NH, DK)), sds((TOK, NH, DV)), sds((TOK, NH, DK))],
        10,
        [
            vm((NH, TOK, DK), B16),
            vm((NH, TOK, DV), B16),
            vm((NH, TOK, DK), B16),
            vm((NH, TOK, DK), B16),
        ],
    )(idx, *back_in, *later_in, qdq, key)
    return dq, dk, dv, da


def solution(mesh):
    torus = Mesh(mesh.devices.reshape(4, 4, 4, 2), (Y, Z, X, H))
    by_token = P(SEQ, H, None)
    placed = (
        by_token,
        by_token,
        by_token,
        P(SEQ + (H,), None, None),
        by_token,
        P(SEQ, H, None, None),
    )
    return jax.shard_map(
        whole, mesh=torus, in_specs=placed, out_specs=(by_token,) * 4, check_vma=False
    )
```

```python
import jax
import jax.numpy as jnp
from jax import lax
from jax.experimental import pallas as pl
from jax.experimental.pallas import tpu as pltpu
from jax.sharding import Mesh
from jax.sharding import PartitionSpec as P


Y, Z, X, H = "seq_0", "seq_1", "seq_2", "head"
SEQ = (Y, Z, X)
F32 = jnp.float32
B16 = jnp.bfloat16
NN = ((1,), (0,))
NT = ((1,), (1,))
TN = ((0,), (0,))
TOK, NH, DK, DV = 128, 4, 256, 512
GROUPS = 16
SCALE = DK ** (-0.5)


def split(x):
    high = x.astype(B16)
    return high, (x - high.astype(F32)).astype(B16)


def three(x):
    first = x.astype(B16)
    rest = x - first.astype(F32)
    second = rest.astype(B16)
    return first, second, (rest - second.astype(F32)).astype(B16)


def dot(a, b, dims):
    return lax.dot_general(a, b, (dims, ((), ())), preferred_element_type=F32)


def dot2(a, b, dims):
    high, low = split(a)
    return dot(high, b, dims) + dot(low, b, dims)


def dot3(a, b, dims):
    a_high, a_low = split(a)
    b_high, b_low = split(b)
    return dot(a_high, b_high, dims) + (dot(a_low, b_high, dims) + dot(a_high, b_low, dims))


def triangle(upper):
    row = lax.broadcasted_iota(jnp.int32, (TOK, TOK), 0)
    col = lax.broadcasted_iota(jnp.int32, (TOK, TOK), 1)
    return (col >= row) if upper else (col <= row)


def sds(shape, dtype=B16):
    return jax.ShapeDtypeStruct(shape, dtype)


def call(body, outs, n_in, scratch=(), after=()):
    specs = [pl.BlockSpec(memory_space=pltpu.SMEM)]
    specs += [pl.BlockSpec(memory_space=pltpu.VMEM)] * n_in
    specs += [pl.BlockSpec(memory_space=pl.ANY)] * len(after)

    def ordered(*refs):
        return body(*refs[: 1 + n_in], *refs[1 + n_in + len(after) :])

    run = pl.pallas_call(
        ordered,
        out_shape=outs,
        in_specs=specs,
        scratch_shapes=list(scratch),
        compiler_params=pltpu.CompilerParams(vmem_limit_bytes=16 * 1024 * 1024),
    )
    return lambda *operands: run(*operands, *after)


def pack_grad(idx, g, send, keep, scr):
    for h in range(2 * NH):
        scr[h] = g[:, h, :]
    c = idx[3]
    for i in range(NH):
        send[i] = scr[NH * (1 - c) + i]
        keep[i] = scr[NH * c + i]


def pack_rows(idx, a, b, out):
    width = a.shape[-1]
    for h in range(NH):
        out[h, :, :width] = a[:, h, :]
        out[h, :, width:] = b[:, h, :]


def pack_pair(idx, a, b, *rest):
    outs, scr = rest[:4], rest[4]
    pack_rows(idx, a, b, scr)
    for s in range(4):
        outs[s][...] = scr[(idx[0] + s) % 4]


def join_all(idx, qa, keep, recv, *outs):
    c = idx[3]
    half = TOK // 2
    mine = pl.ds(pl.multiple_of(half * c, half), half)
    theirs = pl.ds(pl.multiple_of(half * (1 - c), half), half)
    for s in range(4):
        h = (idx[0] + s) % 4
        outs[s][:, : 2 * DK] = qa[h]
        outs[s][mine, 2 * DK :] = keep[h]
        outs[s][theirs, 2 * DK :] = recv[h]


def query_part(idx, *refs):
    qag, kv = refs[0:4], refs[4:8]
    check = refs[8]
    dq_out, qdq_out = refs[9:11]
    kv_out = refs[11:15]
    scr = refs[15]
    low = triangle(False)
    tri = low.astype(B16)
    for s in range(4):
        h = (idx[0] + s) % 4
        q = qag[s][:, :DK].astype(F32)
        cum = dot(tri, qag[s][:, DK : 2 * DK], NN)
        k = kv[s][:, :DK].astype(F32)
        g = qag[s][:, 2 * DK :]
        scores = jnp.where(low, dot(g, kv[s][:, DK:], NT), 0.0)
        reached = dot(g, check[0, h], NT) + dot3(scores, k * jnp.exp(-cum), NN)
        dq = SCALE * jnp.exp(cum) * reached
        scr[h] = dq
        qdq = q * dq
        qdq_out[h] = qdq
        total = jnp.sum(qdq, axis=0, keepdims=True)
        kv_out[s][:TOK, :] = kv[s][...]
        for i, word in enumerate(three(total)):
            kv_out[s][TOK:, DK * i : DK * (i + 1)] = jnp.broadcast_to(word, (16, DK))
    for h in range(NH):
        dq_out[:, h, :] = scr[h].astype(B16)


def line_cum(qa, cum_scr):
    tri = triangle(False).astype(B16)
    base = jnp.zeros((1, DK), F32)
    for j in range(4):
        rows = slice(TOK * j, TOK * (j + 1))
        cum = dot(tri, qa[rows, DK:], NN) + base
        base = cum[TOK - 1 :, :]
        cum_scr[rows, :] = cum
    return base


def line_state(idx, *refs):
    qag = refs[0:4]
    chunks = refs[4:8]
    qa_out, g_out = refs[8:10]
    acc, cum_scr = refs[10:12]
    x, z = idx[0], idx[1]
    for s in range(4):
        j = (x - s + 4) % 4
        rows = pl.ds(pl.multiple_of(TOK * j, TOK), TOK)
        qa_out[rows, :] = qag[s][:, : 2 * DK]
        g_out[rows, :] = qag[s][:, 2 * DK :]
    base = line_cum(qa_out, cum_scr)
    rise = qa_out[:, :DK].astype(F32) * jnp.exp(cum_scr[...])
    high, lo = split(SCALE * rise)
    g = g_out[...]
    acc[...] = dot(g, high, TN) + dot(g, lo, TN)
    for s in range(4):
        at = pl.multiple_of(TOK * ((z + s) % 4), TOK)
        chunks[s][:TOK, :] = acc[pl.ds(at, TOK), :]
        chunks[s][TOK:, :] = jnp.broadcast_to(base, (8, DK))


def scan_z(idx, *refs):
    parts = refs[0:4]
    total, suffix = refs[4:6]
    scr = refs[6]
    z = idx[1]
    for s in range(4):
        scr[(z - s + 4) % 4] = parts[s][...]
    state = jnp.zeros((TOK, DK), F32)
    logs = jnp.zeros((1, DK), F32)
    for j in reversed(range(4)):
        suffix[j, :TOK, :] = state
        suffix[j, TOK:, :] = jnp.broadcast_to(logs, (8, DK))
        own = scr[j, TOK : TOK + 1, :]
        state = jnp.exp(own) * state + scr[j, :TOK, :]
        logs = logs + own
    total[:TOK, :] = state
    total[TOK:, :] = jnp.broadcast_to(logs, (8, DK))


def scan_y(idx, *refs):
    parts, suffix = refs[0:4], refs[4]
    outs, token = refs[5:9], refs[9]
    scr = refs[10]
    y, z = idx[2], idx[1]
    token[...] = jnp.zeros((8, 128), F32)
    for s in range(4):
        scr[(y - s + 4) % 4] = parts[s][...]
    state = jnp.zeros((TOK, DK), F32)
    for j in (3, 2, 1):
        joined = jnp.exp(scr[j, TOK : TOK + 1, :]) * state + scr[j, :TOK, :]
        state = jnp.where(j > y, joined, state)
    for s in range(4):
        j = (z + s) % 4
        outs[s][...] = suffix[j, :TOK, :] + jnp.exp(suffix[j, TOK : TOK + 1, :]) * state


def near_part(idx, *refs):
    qa, g = refs[0:2]
    kv = refs[2:6]
    dk_near, dv_near, k_end, ends, v_out, k_out = refs[6:12]
    rise, cum = refs[12:14]
    last = line_cum(qa, cum)
    x = idx[0]
    for s in range(4):
        j = (x - s + 4) % 4
        rows = pl.ds(pl.multiple_of(TOK * j, TOK), TOK)
        k_out[rows, :] = kv[s][:TOK, :DK]
        v_out[rows, :] = kv[s][:TOK, DK:]
    rise[...] = SCALE * qa[:, :DK].astype(F32) * jnp.exp(cum[...])
    end = jnp.exp(last - cum[...])
    ends[...] = end
    k_end[...] = k_out[...].astype(F32) * end
    upper = triangle(True)
    for j in range(4):
        rows = slice(TOK * j, TOK * (j + 1))
        width = 4 * TOK - TOK * j
        later = slice(TOK * j, 4 * TOK)
        fall = jnp.exp(-cum[rows, :])
        keep = lax.broadcasted_iota(jnp.int32, (TOK, width), 1) >= lax.broadcasted_iota(
            jnp.int32, (TOK, width), 0
        )
        scores = jnp.where(keep, dot(v_out[rows, :], g[later, :], NT), 0.0)
        dk_near[rows, :] = fall * dot3(scores, rise[later, :], NN)
        k_fall = k_out[rows, :].astype(F32) * fall
        affinity = jnp.where(keep, dot3(k_fall, rise[later, :], NT), 0.0)
        dv_near[rows, :] = dot2(affinity, g[later, :], NN)


def far_part(idx, *refs):
    parts = refs[0:4]
    kv = refs[4:8]
    dk_near, dv_near, k_end, ends, v, k = refs[8:14]
    outs = refs[14:18]
    sums = refs[18]
    state, scr, total = refs[19:22]
    x, z = idx[0], idx[1]
    for s in range(4):
        j = (z - s + 4) % 4
        state[pl.ds(pl.multiple_of(TOK * j, TOK), TOK), :] = parts[s][...]
    high, lo = split(state[...])
    reached = dot(v[...], high, NN) + dot(v[...], lo, NN)
    dk = dk_near[...] + ends[...] * reached
    e_high, e_low = split(k_end[...])
    dv = dv_near[...] + (
        dot(e_high, high, NT) + (dot(e_low, high, NT) + dot(e_high, lo, NT))
    )
    kdk = k[...].astype(F32) * dk
    group = lax.broadcasted_iota(jnp.int32, (GROUPS, TOK), 0)
    token = lax.broadcasted_iota(jnp.int32, (GROUPS, TOK), 1)
    after = (token >= (group + 1) * (TOK // GROUPS)).astype(B16)
    for j in range(4):
        rows = slice(TOK * j, TOK * (j + 1))
        part_high, part_low = split(kdk[rows, :])
        ahead = three(dot(after, part_high, NN) + dot(after, part_low, NN))
        scr[j, :TOK, :DK] = dk[rows, :].astype(B16)
        scr[j, :TOK, DK:] = dv[rows, :].astype(B16)
        for i in range(3):
            scr[j, TOK:, DK * i : DK * (i + 1)] = ahead[i]
        total[j : j + 1, :] = -jnp.sum(kdk[rows, :], axis=0, keepdims=True)
    for s in range(4):
        j = (x - s + 4) % 4
        tot = (
            kv[s][TOK : TOK + 1, :DK].astype(F32)
            + kv[s][TOK : TOK + 1, DK : 2 * DK].astype(F32)
            + kv[s][TOK : TOK + 1, 2 * DK :].astype(F32)
        )
        total[pl.ds(j, 1), :] = total[pl.ds(j, 1), :] + tot
    for j in range(4):
        sums[0, 2 * j : 2 * j + 1, :] = total[j : j + 1, :128]
        sums[0, 2 * j + 1 : 2 * j + 2, :] = total[j : j + 1, 128:]
    block = sums[0]
    for d in range(1, 64):
        sums[d] = block
    for s in range(4):
        outs[s][...] = scr[(x + s) % 4]


def final_part(idx, *refs):
    parts = refs[0:4]
    qdq, key = refs[4:6]
    dk_out, dv_out, da_part = refs[6:9]
    s_dk, s_dv, s_k = refs[9:12]
    x = idx[0]
    for h in range(NH):
        s_k[h] = key[:, h, :]
    row = lax.broadcasted_iota(jnp.int32, (TOK, TOK), 0)
    col = lax.broadcasted_iota(jnp.int32, (TOK, TOK), 1)
    size = TOK // GROUPS
    upper = (col >= row).astype(B16)
    inner = ((col >= row) & (col // size == row // size)).astype(B16)
    pick_row = lax.broadcasted_iota(jnp.int32, (TOK, GROUPS), 0)
    pick_col = lax.broadcasted_iota(jnp.int32, (TOK, GROUPS), 1)
    pick = (pick_row // size == pick_col).astype(B16)
    for s in range(4):
        h = (x - s + 4) % 4
        dk = parts[s][:TOK, :DK]
        s_dk[h] = dk
        s_dv[h] = parts[s][:TOK, DK:]
        q_high, q_low = split(qdq[h])
        k_high, k_low = split(s_k[h].astype(F32) * dk.astype(F32))
        ahead = (
            dot(pick, parts[s][TOK:, :DK], NN)
            + dot(pick, parts[s][TOK:, DK : 2 * DK], NN)
            + dot(pick, parts[s][TOK:, 2 * DK :], NN)
        )
        da_part[h] = (
            (dot(upper, q_high, NN) + dot(upper, q_low, NN))
            - (dot(inner, k_high, NN) + dot(inner, k_low, NN))
            - ahead
        )
    for h in range(NH):
        dk_out[:, h, :] = s_dk[h]
        dv_out[:, h, :] = s_dv[h]


def decay_part(idx, da_part, sums, da_out):
    x, line = idx[0], idx[2] * 4 + idx[1]
    segment = lax.broadcasted_iota(jnp.int32, (8, 128), 0) // 2
    for h in range(NH):
        acc = jnp.zeros((8, 128), F32)
        for l in range(16):
            counted = (l > line) | ((l == line) & (segment > x))
            acc = acc + jnp.where(counted, sums[4 * l + h], 0.0)
        first = acc[0:1] + acc[2:3] + acc[4:5] + acc[6:7]
        second = acc[1:2] + acc[3:4] + acc[5:6] + acc[7:8]
        later = jnp.concatenate([first, second], axis=1)
        da_out[:, h, :] = (da_part[h] + later).astype(B16)


def shifted(value, axis, s):
    return lax.ppermute(value, axis, [(i, (i + s) % 4) for i in range(4)])


def spread(parts, axis):
    moved = [parts[0]]
    for s in (1, 2, 3):
        moved.append(shifted(parts[s], axis, s))
    return moved


def whole(query, key, value, out_grad, log_decay, checkpoints):
    x, z, y, c = (lax.axis_index(axis) for axis in (X, Z, Y, H))
    idx = jnp.stack([x, z, y, c]).astype(jnp.int32)
    vm = pltpu.VMEM

    half = TOK // 2
    send, keep = call(
        pack_grad, [sds((NH, half, DV))] * 2, 1, [vm((2 * NH, half, DV), B16)]
    )(idx, out_grad)
    recv = lax.ppermute(send, H, [(0, 1), (1, 0)])
    qa = call(pack_rows, sds((NH, TOK, 2 * DK)), 2, ())(idx, query, log_decay)
    qag = call(join_all, [sds((TOK, 2 * DK + DV))] * 4, 3, ())(idx, qa, keep, recv)
    qag_line = spread(qag, X)
    kv = call(
        pack_pair, [sds((TOK, DK + DV))] * 4, 2, [vm((NH, TOK, DK + DV), B16)]
    )(idx, key, value)
    res = call(
        query_part,
        [sds((TOK, NH, DK)), sds((NH, TOK, DK), F32)] + [sds((TOK + 16, DK + DV))] * 4,
        9,
        [vm((NH, TOK, DK), F32)],
    )(idx, *qag, *kv, checkpoints)
    dq, qdq, kv = res[0], res[1], res[2:]
    res = call(
        line_state,
        [sds((TOK + 8, DK), F32)] * 4
        + [sds((4 * TOK, 2 * DK)), sds((4 * TOK, DV))],
        4,
        [vm((DV, DK), F32), vm((4 * TOK, DK), F32)],
        (qdq,),
    )(idx, *qag_line)
    chunks, qa_rows, g_rows = res[:4], res[4], res[5]
    z_in = spread(chunks, Z)
    kv_line = spread(kv, X)
    total, suffix = call(
        scan_z,
        [sds((TOK + 8, DK), F32), sds((4, TOK + 8, DK), F32)],
        4,
        [vm((4, TOK + 8, DK), F32)],
    )(idx, *z_in)
    y_in = spread([total] * 4, Y)
    *carry, token = call(
        scan_y, [sds((TOK, DK), F32)] * 4 + [sds((8, 128), F32)], 5, [vm((4, TOK + 8, DK), F32)]
    )(idx, *y_in, suffix)
    carry_in = spread(carry, Z)
    near = call(
        near_part,
        [
            sds((4 * TOK, DK), F32),
            sds((4 * TOK, DV), F32),
            sds((4 * TOK, DK), F32),
            sds((4 * TOK, DK), F32),
            sds((4 * TOK, DV)),
            sds((4 * TOK, DK)),
        ],
        6,
        [vm((4 * TOK, DK), F32)] * 2,
        (token,),
    )(idx, qa_rows, g_rows, *kv_line)
    res = call(
        far_part,
        [sds((TOK + GROUPS, DK + DV))] * 4 + [sds((64, 8, 128), F32)],
        14,
        [vm((DV, DK), F32), vm((4, TOK + GROUPS, DK + DV), B16), vm((4, DK), F32)],
    )(idx, *carry_in, *kv_line, *near)
    back, sums = res[:4], res[4]
    back_in = spread(back, X)
    sums = lax.all_to_all(sums, SEQ, split_axis=0, concat_axis=0, tiled=True)
    dk, dv, da_part = call(
        final_part,
        [sds((TOK, NH, DK)), sds((TOK, NH, DV)), sds((NH, TOK, DK), F32)],
        6,
        [vm((NH, TOK, DK), B16), vm((NH, TOK, DV), B16), vm((NH, TOK, DK), B16)],
    )(idx, *back_in, qdq, key)
    da = call(decay_part, sds((TOK, NH, DK)), 2, ())(idx, da_part, sums)
    return dq, dk, dv, da


def solution(mesh):
    torus = Mesh(mesh.devices.reshape(4, 4, 4, 2), (Y, Z, X, H))
    by_token = P(SEQ, H, None)
    placed = (
        by_token,
        by_token,
        by_token,
        P(SEQ + (H,), None, None),
        by_token,
        P(SEQ, H, None, None),
    )
    return jax.shard_map(
        whole, mesh=torus, in_specs=placed, out_specs=(by_token,) * 4, check_vma=False
    )
```

```python
import jax
import jax.numpy as jnp
from jax import lax
from jax.experimental import pallas as pl
from jax.experimental.pallas import tpu as pltpu
from jax.sharding import Mesh
from jax.sharding import PartitionSpec as P


Y, Z, X, H = "seq_0", "seq_1", "seq_2", "head"
SEQ = (Y, Z, X)
F32 = jnp.float32
B16 = jnp.bfloat16
NN = ((1,), (0,))
NT = ((1,), (1,))
TN = ((0,), (0,))
TOK, NH, DK, DV = 128, 4, 256, 512
GROUPS = 16
SCALE = DK ** (-0.5)


def split(x):
    high = x.astype(B16)
    return high, (x - high.astype(F32)).astype(B16)


def three(x):
    first = x.astype(B16)
    rest = x - first.astype(F32)
    second = rest.astype(B16)
    return first, second, (rest - second.astype(F32)).astype(B16)


def dot(a, b, dims):
    return lax.dot_general(a, b, (dims, ((), ())), preferred_element_type=F32)


def dot2(a, b, dims):
    high, low = split(a)
    return dot(high, b, dims) + dot(low, b, dims)


def dot3(a, b, dims):
    a_high, a_low = split(a)
    b_high, b_low = split(b)
    return dot(a_high, b_high, dims) + (dot(a_low, b_high, dims) + dot(a_high, b_low, dims))


def triangle(upper):
    row = lax.broadcasted_iota(jnp.int32, (TOK, TOK), 0)
    col = lax.broadcasted_iota(jnp.int32, (TOK, TOK), 1)
    return (col >= row) if upper else (col <= row)


def sds(shape, dtype=B16):
    return jax.ShapeDtypeStruct(shape, dtype)


def call(body, outs, n_in, scratch=(), after=()):
    specs = [pl.BlockSpec(memory_space=pltpu.SMEM)]
    specs += [pl.BlockSpec(memory_space=pltpu.VMEM)] * n_in
    specs += [pl.BlockSpec(memory_space=pl.ANY)] * len(after)

    def ordered(*refs):
        return body(*refs[: 1 + n_in], *refs[1 + n_in + len(after) :])

    run = pl.pallas_call(
        ordered,
        out_shape=outs,
        in_specs=specs,
        scratch_shapes=list(scratch),
        compiler_params=pltpu.CompilerParams(vmem_limit_bytes=16 * 1024 * 1024),
    )
    return lambda *operands: run(*operands, *after)


def pack_grad(idx, g, send, keep, scr):
    scr[...] = jnp.swapaxes(g[...], 0, 1)
    c = idx[3]
    for i in range(NH):
        send[i] = scr[NH * (1 - c) + i]
        keep[i] = scr[NH * c + i]


def pack_rows(idx, a, b, out):
    width = a.shape[-1]
    out[:, :, :width] = jnp.swapaxes(a[...], 0, 1)
    out[:, :, width:] = jnp.swapaxes(b[...], 0, 1)


def pack_pair(idx, a, b, *rest):
    outs, scr = rest[:4], rest[4]
    pack_rows(idx, a, b, scr)
    for s in range(4):
        outs[s][...] = scr[(idx[0] + s) % 4]


def join_all(idx, qa, keep, recv, *outs):
    c = idx[3]
    half = TOK // 2
    mine = pl.ds(pl.multiple_of(half * c, half), half)
    theirs = pl.ds(pl.multiple_of(half * (1 - c), half), half)
    for s in range(4):
        h = (idx[0] + s) % 4
        outs[s][:, : 2 * DK] = qa[h]
        outs[s][mine, 2 * DK :] = keep[h]
        outs[s][theirs, 2 * DK :] = recv[h]


def query_part(idx, *refs):
    qag, kv = refs[0:4], refs[4:8]
    check = refs[8]
    dq_out, qdq_out = refs[9:11]
    kv_out = refs[11:15]
    scr = refs[15]
    low = triangle(False)
    tri = low.astype(B16)
    for s in range(4):
        h = (idx[0] + s) % 4
        q = qag[s][:, :DK].astype(F32)
        cum = dot(tri, qag[s][:, DK : 2 * DK], NN)
        k = kv[s][:, :DK].astype(F32)
        g = qag[s][:, 2 * DK :]
        scores = jnp.where(low, dot(g, kv[s][:, DK:], NT), 0.0)
        reached = dot(g, check[0, h], NT) + dot3(scores, k * jnp.exp(-cum), NN)
        dq = SCALE * jnp.exp(cum) * reached
        scr[h] = dq
        qdq = q * dq
        qdq_out[h] = qdq
        total = jnp.sum(qdq, axis=0, keepdims=True)
        kv_out[s][:TOK, :] = kv[s][...]
        for i, word in enumerate(three(total)):
            kv_out[s][TOK:, DK * i : DK * (i + 1)] = jnp.broadcast_to(word, (16, DK))
    dq_out[...] = jnp.swapaxes(scr[...].astype(B16), 0, 1)


def line_cum(qa, cum_scr):
    tri = triangle(False).astype(B16)
    base = jnp.zeros((1, DK), F32)
    for j in range(4):
        rows = slice(TOK * j, TOK * (j + 1))
        cum = dot(tri, qa[rows, DK:], NN) + base
        base = cum[TOK - 1 :, :]
        cum_scr[rows, :] = cum
    return base


def line_state(idx, *refs):
    qag = refs[0:4]
    chunks = refs[4:8]
    qa_out, g_out = refs[8:10]
    acc, cum_scr = refs[10:12]
    x, z = idx[0], idx[1]
    for s in range(4):
        j = (x - s + 4) % 4
        rows = pl.ds(pl.multiple_of(TOK * j, TOK), TOK)
        qa_out[rows, :] = qag[s][:, : 2 * DK]
        g_out[rows, :] = qag[s][:, 2 * DK :]
    base = line_cum(qa_out, cum_scr)
    rise = qa_out[:, :DK].astype(F32) * jnp.exp(cum_scr[...])
    high, lo = split(SCALE * rise)
    g = g_out[...]
    acc[...] = dot(g, high, TN) + dot(g, lo, TN)
    for s in range(4):
        at = pl.multiple_of(TOK * ((z + s) % 4), TOK)
        chunks[s][:TOK, :] = acc[pl.ds(at, TOK), :]
        chunks[s][TOK:, :] = jnp.broadcast_to(base, (8, DK))


def scan_z(idx, *refs):
    parts = refs[0:4]
    total, suffix = refs[4:6]
    scr = refs[6]
    z = idx[1]
    for s in range(4):
        scr[(z - s + 4) % 4] = parts[s][...]
    state = jnp.zeros((TOK, DK), F32)
    logs = jnp.zeros((1, DK), F32)
    for j in reversed(range(4)):
        suffix[j, :TOK, :] = state
        suffix[j, TOK:, :] = jnp.broadcast_to(logs, (8, DK))
        own = scr[j, TOK : TOK + 1, :]
        state = jnp.exp(own) * state + scr[j, :TOK, :]
        logs = logs + own
    total[:TOK, :] = state
    total[TOK:, :] = jnp.broadcast_to(logs, (8, DK))


def scan_y(idx, *refs):
    parts, suffix = refs[0:4], refs[4]
    outs, token = refs[5:9], refs[9]
    scr = refs[10]
    y, z = idx[2], idx[1]
    token[...] = jnp.zeros((8, 128), F32)
    for s in range(4):
        scr[(y - s + 4) % 4] = parts[s][...]
    state = jnp.zeros((TOK, DK), F32)
    for j in (3, 2, 1):
        joined = jnp.exp(scr[j, TOK : TOK + 1, :]) * state + scr[j, :TOK, :]
        state = jnp.where(j > y, joined, state)
    for s in range(4):
        j = (z + s) % 4
        outs[s][...] = suffix[j, :TOK, :] + jnp.exp(suffix[j, TOK : TOK + 1, :]) * state


def near_part(idx, *refs):
    qa, g = refs[0:2]
    kv = refs[2:6]
    dk_near, dv_near, k_end, ends, v_out, k_out = refs[6:12]
    rise, cum = refs[12:14]
    last = line_cum(qa, cum)
    x = idx[0]
    for s in range(4):
        j = (x - s + 4) % 4
        rows = pl.ds(pl.multiple_of(TOK * j, TOK), TOK)
        k_out[rows, :] = kv[s][:TOK, :DK]
        v_out[rows, :] = kv[s][:TOK, DK:]
    rise[...] = SCALE * qa[:, :DK].astype(F32) * jnp.exp(cum[...])
    end = jnp.exp(last - cum[...])
    ends[...] = end
    k_end[:, :DK], k_end[:, DK:] = split(k_out[...].astype(F32) * end)
    upper = triangle(True)
    for j in range(4):
        rows = slice(TOK * j, TOK * (j + 1))
        width = 4 * TOK - TOK * j
        later = slice(TOK * j, 4 * TOK)
        fall = jnp.exp(-cum[rows, :])
        keep = lax.broadcasted_iota(jnp.int32, (TOK, width), 1) >= lax.broadcasted_iota(
            jnp.int32, (TOK, width), 0
        )
        scores = jnp.where(keep, dot(v_out[rows, :], g[later, :], NT), 0.0)
        dk_near[rows, :] = fall * dot3(scores, rise[later, :], NN)
        k_fall = k_out[rows, :].astype(F32) * fall
        affinity = jnp.where(keep, dot3(k_fall, rise[later, :], NT), 0.0)
        dv_near[rows, :] = dot2(affinity, g[later, :], NN)


def far_part(idx, *refs):
    parts = refs[0:4]
    kv = refs[4:8]
    dk_near, dv_near, k_end, ends, v, k = refs[8:14]
    outs = refs[14:18]
    sums = refs[18]
    state, scr, total = refs[19:22]
    x, z = idx[0], idx[1]
    for s in range(4):
        j = (z - s + 4) % 4
        state[pl.ds(pl.multiple_of(TOK * j, TOK), TOK), :] = parts[s][...]
    high, lo = split(state[...])
    reached = dot(v[...], high, NN) + dot(v[...], lo, NN)
    dk = dk_near[...] + ends[...] * reached
    e_high, e_low = k_end[:, :DK], k_end[:, DK:]
    dv = dv_near[...] + (
        dot(e_high, high, NT) + (dot(e_low, high, NT) + dot(e_high, lo, NT))
    )
    kdk = k[...].astype(F32) * dk
    group = lax.broadcasted_iota(jnp.int32, (GROUPS, TOK), 0)
    token = lax.broadcasted_iota(jnp.int32, (GROUPS, TOK), 1)
    after = (token >= (group + 1) * (TOK // GROUPS)).astype(B16)
    for j in range(4):
        total[j : j + 1, :] = -jnp.sum(
            kdk[TOK * j : TOK * (j + 1), :], axis=0, keepdims=True
        )
    for s in range(4):
        j = (x - s + 4) % 4
        tot = (
            kv[s][TOK : TOK + 1, :DK].astype(F32)
            + kv[s][TOK : TOK + 1, DK : 2 * DK].astype(F32)
            + kv[s][TOK : TOK + 1, 2 * DK :].astype(F32)
        )
        total[pl.ds(j, 1), :] = total[pl.ds(j, 1), :] + tot
    running = jnp.zeros((1, DK), F32)
    for j in reversed(range(4)):
        rows = slice(TOK * j, TOK * (j + 1))
        part_high, part_low = split(kdk[rows, :])
        ahead = three(running - (dot(after, part_high, NN) + dot(after, part_low, NN)))
        running = running + total[j : j + 1, :]
        scr[j, :TOK, :DK] = dk[rows, :].astype(B16)
        scr[j, :TOK, DK:] = dv[rows, :].astype(B16)
        for i in range(3):
            scr[j, TOK:, DK * i : DK * (i + 1)] = ahead[i]
    block = jnp.concatenate([running[:, :128], running[:, 128:]], axis=0)
    for d in range(64):
        sums[d] = block
    for s in range(4):
        outs[s][...] = scr[(x + s) % 4]


def final_part(idx, *refs):
    parts = refs[0:4]
    qdq, key = refs[4:6]
    dk_out, dv_out, da_part = refs[6:9]
    s_dk, s_dv, s_k, s_da = refs[9:13]
    x = idx[0]
    s_k[...] = jnp.swapaxes(key[...], 0, 1)
    row = lax.broadcasted_iota(jnp.int32, (TOK, TOK), 0)
    col = lax.broadcasted_iota(jnp.int32, (TOK, TOK), 1)
    size = TOK // GROUPS
    upper = (col >= row).astype(B16)
    inner = ((col >= row) & (col // size == row // size)).astype(B16)
    pick_row = lax.broadcasted_iota(jnp.int32, (TOK, GROUPS), 0)
    pick_col = lax.broadcasted_iota(jnp.int32, (TOK, GROUPS), 1)
    pick = (pick_row // size == pick_col).astype(B16)
    for s in range(4):
        h = (x - s + 4) % 4
        dk = parts[s][:TOK, :DK]
        s_dk[h] = dk
        s_dv[h] = parts[s][:TOK, DK:]
        q_high, q_low = split(qdq[h])
        k_high, k_low = split(s_k[h].astype(F32) * dk.astype(F32))
        ahead = (
            dot(pick, parts[s][TOK:, :DK], NN)
            + dot(pick, parts[s][TOK:, DK : 2 * DK], NN)
            + dot(pick, parts[s][TOK:, 2 * DK :], NN)
        )
        s_da[h] = (
            (dot(upper, q_high, NN) + dot(upper, q_low, NN))
            - (dot(inner, k_high, NN) + dot(inner, k_low, NN))
            + ahead
        )
    dk_out[...] = jnp.swapaxes(s_dk[...], 0, 1)
    dv_out[...] = jnp.swapaxes(s_dv[...], 0, 1)
    da_part[...] = jnp.swapaxes(s_da[...], 0, 1)


def decay_part(idx, da_part, sums, da_out):
    line = idx[2] * 4 + idx[1]
    later = []
    for h in range(NH):
        acc = jnp.zeros((2, 128), F32)
        for l in range(1, 16):
            acc = acc + jnp.where(l > line, sums[4 * l + h], 0.0)
        later.append(jnp.concatenate([acc[0:1], acc[1:2]], axis=1))
    da_out[...] = (da_part[...] + jnp.concatenate(later, axis=0)[None]).astype(B16)


def shifted(value, axis, s):
    return lax.ppermute(value, axis, [(i, (i + s) % 4) for i in range(4)])


def spread(parts, axis):
    moved = [parts[0]]
    for s in (1, 2, 3):
        moved.append(shifted(parts[s], axis, s))
    return moved


def whole(query, key, value, out_grad, log_decay, checkpoints):
    x, z, y, c = (lax.axis_index(axis) for axis in (X, Z, Y, H))
    idx = jnp.stack([x, z, y, c]).astype(jnp.int32)
    vm = pltpu.VMEM

    half = TOK // 2
    send, keep = call(
        pack_grad, [sds((NH, half, DV))] * 2, 1, [vm((2 * NH, half, DV), B16)]
    )(idx, out_grad)
    recv = lax.ppermute(send, H, [(0, 1), (1, 0)])
    qa = call(pack_rows, sds((NH, TOK, 2 * DK)), 2, ())(idx, query, log_decay)
    qag = call(join_all, [sds((TOK, 2 * DK + DV))] * 4, 3, ())(idx, qa, keep, recv)
    qag_line = spread(qag, X)
    kv = call(
        pack_pair, [sds((TOK, DK + DV))] * 4, 2, [vm((NH, TOK, DK + DV), B16)]
    )(idx, key, value)
    res = call(
        query_part,
        [sds((TOK, NH, DK)), sds((NH, TOK, DK), F32)] + [sds((TOK + 16, DK + DV))] * 4,
        9,
        [vm((NH, TOK, DK), F32)],
    )(idx, *qag, *kv, checkpoints)
    dq, qdq, kv = res[0], res[1], res[2:]
    res = call(
        line_state,
        [sds((TOK + 8, DK), F32)] * 4
        + [sds((4 * TOK, 2 * DK)), sds((4 * TOK, DV))],
        4,
        [vm((DV, DK), F32), vm((4 * TOK, DK), F32)],
        (qdq,),
    )(idx, *qag_line)
    chunks, qa_rows, g_rows = res[:4], res[4], res[5]
    z_in = spread(chunks, Z)
    kv_line = spread(kv, X)
    total, suffix = call(
        scan_z,
        [sds((TOK + 8, DK), F32), sds((4, TOK + 8, DK), F32)],
        4,
        [vm((4, TOK + 8, DK), F32)],
    )(idx, *z_in)
    y_in = spread([total] * 4, Y)
    *carry, token = call(
        scan_y, [sds((TOK, DK), F32)] * 4 + [sds((8, 128), F32)], 5, [vm((4, TOK + 8, DK), F32)]
    )(idx, *y_in, suffix)
    carry_in = spread(carry, Z)
    near = call(
        near_part,
        [
            sds((4 * TOK, DK), F32),
            sds((4 * TOK, DV), F32),
            sds((4 * TOK, 2 * DK)),
            sds((4 * TOK, DK), F32),
            sds((4 * TOK, DV)),
            sds((4 * TOK, DK)),
        ],
        6,
        [vm((4 * TOK, DK), F32)] * 2,
        (token,),
    )(idx, qa_rows, g_rows, *kv_line)
    res = call(
        far_part,
        [sds((TOK + GROUPS, DK + DV))] * 4 + [sds((64, 2, 128), F32)],
        14,
        [vm((DV, DK), F32), vm((4, TOK + GROUPS, DK + DV), B16), vm((4, DK), F32)],
    )(idx, *carry_in, *kv_line, *near)
    back, sums = res[:4], res[4]
    back_in = spread(back, X)
    sums = lax.all_to_all(sums, SEQ, split_axis=0, concat_axis=0, tiled=True)
    dk, dv, da_part = call(
        final_part,
        [sds((TOK, NH, DK)), sds((TOK, NH, DV)), sds((TOK, NH, DK), F32)],
        6,
        [
            vm((NH, TOK, DK), B16),
            vm((NH, TOK, DV), B16),
            vm((NH, TOK, DK), B16),
            vm((NH, TOK, DK), F32),
        ],
    )(idx, *back_in, qdq, key)
    da = call(decay_part, sds((TOK, NH, DK)), 2, ())(idx, da_part, sums)
    return dq, dk, dv, da


def solution(mesh):
    torus = Mesh(mesh.devices.reshape(4, 4, 4, 2), (Y, Z, X, H))
    by_token = P(SEQ, H, None)
    placed = (
        by_token,
        by_token,
        by_token,
        P(SEQ + (H,), None, None),
        by_token,
        P(SEQ, H, None, None),
    )
    return jax.shard_map(
        whole, mesh=torus, in_specs=placed, out_specs=(by_token,) * 4, check_vma=False
    )
```

```python
import jax
import jax.numpy as jnp
from jax import lax
from jax.experimental import pallas as pl
from jax.experimental.pallas import tpu as pltpu
from jax.sharding import Mesh
from jax.sharding import PartitionSpec as P


Y, Z, X, H = "seq_0", "seq_1", "seq_2", "head"
SEQ = (Y, Z, X)
F32 = jnp.float32
B16 = jnp.bfloat16
NN = ((1,), (0,))
NT = ((1,), (1,))
TN = ((0,), (0,))
TOK, NH, DK, DV = 128, 4, 256, 512
GROUPS = 16
SCALE = DK ** (-0.5)


def split(x):
    high = x.astype(B16)
    return high, (x - high.astype(F32)).astype(B16)


def three(x):
    first = x.astype(B16)
    rest = x - first.astype(F32)
    second = rest.astype(B16)
    return first, second, (rest - second.astype(F32)).astype(B16)


def dot(a, b, dims):
    return lax.dot_general(a, b, (dims, ((), ())), preferred_element_type=F32)


def dot2(a, b, dims):
    high, low = split(a)
    return dot(high, b, dims) + dot(low, b, dims)


def dot3(a, b, dims):
    a_high, a_low = split(a)
    b_high, b_low = split(b)
    return dot(a_high, b_high, dims) + (dot(a_low, b_high, dims) + dot(a_high, b_low, dims))


def triangle(upper):
    row = lax.broadcasted_iota(jnp.int32, (TOK, TOK), 0)
    col = lax.broadcasted_iota(jnp.int32, (TOK, TOK), 1)
    return (col >= row) if upper else (col <= row)


def sds(shape, dtype=B16):
    return jax.ShapeDtypeStruct(shape, dtype)


def call(body, outs, n_in, scratch=(), after=()):
    specs = [pl.BlockSpec(memory_space=pltpu.SMEM)]
    specs += [pl.BlockSpec(memory_space=pltpu.VMEM)] * n_in
    specs += [pl.BlockSpec(memory_space=pl.ANY)] * len(after)

    def ordered(*refs):
        return body(*refs[: 1 + n_in], *refs[1 + n_in + len(after) :])

    run = pl.pallas_call(
        ordered,
        out_shape=outs,
        in_specs=specs,
        scratch_shapes=list(scratch),
        compiler_params=pltpu.CompilerParams(vmem_limit_bytes=16 * 1024 * 1024),
    )
    return lambda *operands: run(*operands, *after)


def pack_first(idx, grad, query, decay, *refs):
    outs, send, keep = refs[0:4], refs[4], refs[5]
    g, q, a, heads, scr, sems = refs[6:12]
    copies = [
        pltpu.make_async_copy(source, target, sems.at[i])
        for i, (source, target) in enumerate(((grad, g), (query, q), (decay, a)))
    ]
    for copy in copies:
        copy.start()
    x, c = idx[0], idx[3]
    copies[0].wait()
    heads[...] = jnp.swapaxes(g[...], 0, 1)
    for i in range(NH):
        send[i] = heads[NH * (1 - c) + i]
        keep[i] = heads[NH * c + i]
    copies[1].wait()
    scr[:, :, :DK] = jnp.swapaxes(q[...], 0, 1)
    copies[2].wait()
    scr[:, :, DK:] = jnp.swapaxes(a[...], 0, 1)
    for s in range(4):
        outs[s][...] = scr[(x + s) % 4]


def pack_rows(a, b, out):
    width = a.shape[-1]
    out[:, :, :width] = jnp.swapaxes(a[...], 0, 1)
    out[:, :, width:] = jnp.swapaxes(b[...], 0, 1)


def pack_pair(idx, a, b, *rest):
    outs, scr = rest[:4], rest[4]
    pack_rows(a, b, scr)
    for s in range(4):
        outs[s][...] = scr[(idx[0] + s) % 4]


def join_grad(idx, keep, recv, *outs):
    c = idx[3]
    half = TOK // 2
    mine = pl.ds(pl.multiple_of(half * c, half), half)
    theirs = pl.ds(pl.multiple_of(half * (1 - c), half), half)
    for s in range(4):
        h = (idx[0] + s) % 4
        outs[s][mine, :] = keep[h]
        outs[s][theirs, :] = recv[h]


def query_part(idx, *refs):
    qa, gr, kv = refs[0:4], refs[4:8], refs[8:12]
    check = refs[12]
    dq_out, qdq_out = refs[13:15]
    kv_out = refs[15:19]
    scr = refs[19]
    low = triangle(False)
    tri = low.astype(B16)
    for s in range(4):
        h = (idx[0] + s) % 4
        q = qa[s][:, :DK].astype(F32)
        cum = dot(tri, qa[s][:, DK:], NN)
        k = kv[s][:, :DK].astype(F32)
        g = gr[s][...]
        scores = jnp.where(low, dot(g, kv[s][:, DK:], NT), 0.0)
        reached = dot(g, check[0, h], NT) + dot3(scores, k * jnp.exp(-cum), NN)
        dq = SCALE * jnp.exp(cum) * reached
        scr[h] = dq
        qdq = q * dq
        qdq_out[h] = qdq
        total = jnp.sum(qdq, axis=0, keepdims=True)
        kv_out[s][:TOK, :] = kv[s][...]
        for i, word in enumerate(three(total)):
            kv_out[s][TOK:, DK * i : DK * (i + 1)] = jnp.broadcast_to(word, (16, DK))
    dq_out[...] = jnp.swapaxes(scr[...].astype(B16), 0, 1)


def line_cum(qa, cum_scr):
    tri = triangle(False).astype(B16)
    base = jnp.zeros((1, DK), F32)
    for j in range(4):
        rows = slice(TOK * j, TOK * (j + 1))
        cum = dot(tri, qa[rows, DK:], NN) + base
        base = cum[TOK - 1 :, :]
        cum_scr[rows, :] = cum
    return base


def line_state(idx, *refs):
    qa, gr = refs[0:4], refs[4:8]
    chunks = refs[8:12]
    qa_out, g_out = refs[12:14]
    acc, cum_scr = refs[14:16]
    x, z = idx[0], idx[1]
    for s in range(4):
        j = (x - s + 4) % 4
        rows = pl.ds(pl.multiple_of(TOK * j, TOK), TOK)
        qa_out[rows, :] = qa[s][...]
        g_out[rows, :] = gr[s][...]
    base = line_cum(qa_out, cum_scr)
    rise = qa_out[:, :DK].astype(F32) * jnp.exp(cum_scr[...])
    high, lo = split(SCALE * rise)
    g = g_out[...]
    acc[...] = dot(g, high, TN) + dot(g, lo, TN)
    for s in range(4):
        at = pl.multiple_of(TOK * ((z + s) % 4), TOK)
        chunks[s][:TOK, :] = acc[pl.ds(at, TOK), :]
        chunks[s][TOK:, :] = jnp.broadcast_to(base, (8, DK))


def scan_z(idx, *refs):
    parts = refs[0:4]
    total, suffix = refs[4:6]
    scr = refs[6]
    z = idx[1]
    for s in range(4):
        scr[(z - s + 4) % 4] = parts[s][...]
    state = jnp.zeros((TOK, DK), F32)
    logs = jnp.zeros((1, DK), F32)
    for j in reversed(range(4)):
        suffix[j, :TOK, :] = state
        suffix[j, TOK:, :] = jnp.broadcast_to(logs, (8, DK))
        own = scr[j, TOK : TOK + 1, :]
        state = jnp.exp(own) * state + scr[j, :TOK, :]
        logs = logs + own
    total[:TOK, :] = state
    total[TOK:, :] = jnp.broadcast_to(logs, (8, DK))


def scan_y(idx, *refs):
    parts, suffix = refs[0:4], refs[4]
    outs, token = refs[5:9], refs[9]
    scr = refs[10]
    y, z = idx[2], idx[1]
    token[...] = jnp.zeros((8, 128), F32)
    for s in range(4):
        scr[(y - s + 4) % 4] = parts[s][...]
    state = jnp.zeros((TOK, DK), F32)
    for j in (3, 2, 1):
        joined = jnp.exp(scr[j, TOK : TOK + 1, :]) * state + scr[j, :TOK, :]
        state = jnp.where(j > y, joined, state)
    for s in range(4):
        j = (z + s) % 4
        outs[s][...] = suffix[j, :TOK, :] + jnp.exp(suffix[j, TOK : TOK + 1, :]) * state


def near_part(idx, *refs):
    qa, g = refs[0:2]
    kv = refs[2:6]
    dk_near, dv_near, k_end, ends, v_out, k_out = refs[6:12]
    rise, cum = refs[12:14]
    last = line_cum(qa, cum)
    x = idx[0]
    for s in range(4):
        j = (x - s + 4) % 4
        rows = pl.ds(pl.multiple_of(TOK * j, TOK), TOK)
        k_out[rows, :] = kv[s][:TOK, :DK]
        v_out[rows, :] = kv[s][:TOK, DK:]
    rise[...] = SCALE * qa[:, :DK].astype(F32) * jnp.exp(cum[...])
    end = jnp.exp(last - cum[...])
    ends[...] = end
    k_end[:, :DK], k_end[:, DK:] = split(k_out[...].astype(F32) * end)
    upper = triangle(True)
    for j in range(4):
        rows = slice(TOK * j, TOK * (j + 1))
        width = 4 * TOK - TOK * j
        later = slice(TOK * j, 4 * TOK)
        fall = jnp.exp(-cum[rows, :])
        keep = lax.broadcasted_iota(jnp.int32, (TOK, width), 1) >= lax.broadcasted_iota(
            jnp.int32, (TOK, width), 0
        )
        scores = jnp.where(keep, dot(v_out[rows, :], g[later, :], NT), 0.0)
        dk_near[rows, :] = fall * dot3(scores, rise[later, :], NN)
        k_fall = k_out[rows, :].astype(F32) * fall
        affinity = jnp.where(keep, dot3(k_fall, rise[later, :], NT), 0.0)
        dv_near[rows, :] = dot2(affinity, g[later, :], NN)


def far_part(idx, *refs):
    parts = refs[0:4]
    kv = refs[4:8]
    dk_near, dv_near, k_end, ends, v, k = refs[8:14]
    outs = refs[14:18]
    sums = refs[18]
    state, scr, total = refs[19:22]
    x, z = idx[0], idx[1]
    for s in range(4):
        j = (z - s + 4) % 4
        state[pl.ds(pl.multiple_of(TOK * j, TOK), TOK), :] = parts[s][...]
    high, lo = split(state[...])
    reached = dot(v[...], high, NN) + dot(v[...], lo, NN)
    dk = dk_near[...] + ends[...] * reached
    e_high, e_low = k_end[:, :DK], k_end[:, DK:]
    dv = dv_near[...] + (
        dot(e_high, high, NT) + (dot(e_low, high, NT) + dot(e_high, lo, NT))
    )
    kdk = k[...].astype(F32) * dk
    group = lax.broadcasted_iota(jnp.int32, (GROUPS, TOK), 0)
    token = lax.broadcasted_iota(jnp.int32, (GROUPS, TOK), 1)
    after = (token >= (group + 1) * (TOK // GROUPS)).astype(B16)
    for j in range(4):
        total[j : j + 1, :] = -jnp.sum(
            kdk[TOK * j : TOK * (j + 1), :], axis=0, keepdims=True
        )
    for s in range(4):
        j = (x - s + 4) % 4
        tot = (
            kv[s][TOK : TOK + 1, :DK].astype(F32)
            + kv[s][TOK : TOK + 1, DK : 2 * DK].astype(F32)
            + kv[s][TOK : TOK + 1, 2 * DK :].astype(F32)
        )
        total[pl.ds(j, 1), :] = total[pl.ds(j, 1), :] + tot
    running = jnp.zeros((1, DK), F32)
    for j in reversed(range(4)):
        rows = slice(TOK * j, TOK * (j + 1))
        part_high, part_low = split(kdk[rows, :])
        ahead = three(running - (dot(after, part_high, NN) + dot(after, part_low, NN)))
        running = running + total[j : j + 1, :]
        scr[j, :TOK, :DK] = dk[rows, :].astype(B16)
        scr[j, :TOK, DK:] = dv[rows, :].astype(B16)
        for i in range(3):
            scr[j, TOK:, DK * i : DK * (i + 1)] = ahead[i]
    block = jnp.concatenate([running[:, :128], running[:, 128:]], axis=0)
    for d in range(64):
        sums[d] = block
    for s in range(4):
        outs[s][...] = scr[(x + s) % 4]


def final_part(idx, *refs):
    parts = refs[0:4]
    qdq, key = refs[4:6]
    dk_out, dv_out, da_part = refs[6:9]
    s_dk, s_dv, s_k, s_da = refs[9:13]
    x = idx[0]
    s_k[...] = jnp.swapaxes(key[...], 0, 1)
    row = lax.broadcasted_iota(jnp.int32, (TOK, TOK), 0)
    col = lax.broadcasted_iota(jnp.int32, (TOK, TOK), 1)
    size = TOK // GROUPS
    upper = (col >= row).astype(B16)
    inner = ((col >= row) & (col // size == row // size)).astype(B16)
    pick_row = lax.broadcasted_iota(jnp.int32, (TOK, GROUPS), 0)
    pick_col = lax.broadcasted_iota(jnp.int32, (TOK, GROUPS), 1)
    pick = (pick_row // size == pick_col).astype(B16)
    for s in range(4):
        h = (x - s + 4) % 4
        dk = parts[s][:TOK, :DK]
        s_dk[h] = dk
        s_dv[h] = parts[s][:TOK, DK:]
        q_high, q_low = split(qdq[h])
        k_high, k_low = split(s_k[h].astype(F32) * dk.astype(F32))
        ahead = (
            dot(pick, parts[s][TOK:, :DK], NN)
            + dot(pick, parts[s][TOK:, DK : 2 * DK], NN)
            + dot(pick, parts[s][TOK:, 2 * DK :], NN)
        )
        s_da[h] = (
            (dot(upper, q_high, NN) + dot(upper, q_low, NN))
            - (dot(inner, k_high, NN) + dot(inner, k_low, NN))
            + ahead
        )
    dk_out[...] = jnp.swapaxes(s_dk[...], 0, 1)
    dv_out[...] = jnp.swapaxes(s_dv[...], 0, 1)
    da_part[...] = jnp.swapaxes(s_da[...], 0, 1)


def decay_part(idx, da_part, sums, da_out):
    line = idx[2] * 4 + idx[1]
    later = []
    for h in range(NH):
        acc = jnp.zeros((2, 128), F32)
        for l in range(1, 16):
            acc = acc + jnp.where(l > line, sums[4 * l + h], 0.0)
        later.append(jnp.concatenate([acc[0:1], acc[1:2]], axis=1))
    da_out[...] = (da_part[...] + jnp.concatenate(later, axis=0)[None]).astype(B16)


def shifted(value, axis, s):
    return lax.ppermute(value, axis, [(i, (i + s) % 4) for i in range(4)])


def spread(parts, axis):
    moved = [parts[0]]
    for s in (1, 2, 3):
        moved.append(shifted(parts[s], axis, s))
    return moved


def whole(query, key, value, out_grad, log_decay, checkpoints):
    x, z, y, c = (lax.axis_index(axis) for axis in (X, Z, Y, H))
    idx = jnp.stack([x, z, y, c]).astype(jnp.int32)
    vm = pltpu.VMEM

    half = TOK // 2
    hbm = pl.BlockSpec(memory_space=pltpu.HBM)
    *qa, send, keep = pl.pallas_call(
        pack_first,
        out_shape=[sds((TOK, 2 * DK))] * 4 + [sds((NH, half, DV))] * 2,
        in_specs=[pl.BlockSpec(memory_space=pltpu.SMEM), hbm, hbm, hbm],
        scratch_shapes=[
            vm((half, 2 * NH, DV), B16),
            vm((TOK, NH, DK), B16),
            vm((TOK, NH, DK), B16),
            vm((2 * NH, half, DV), B16),
            vm((NH, TOK, 2 * DK), B16),
            pltpu.SemaphoreType.DMA((3,)),
        ],
        name="pack_first",
        compiler_params=pltpu.CompilerParams(vmem_limit_bytes=16 * 1024 * 1024),
    )(idx, *(pltpu.with_memory_space_constraint(a, pltpu.HBM) for a in (out_grad, query, log_decay)))
    recv = lax.ppermute(send, H, [(0, 1), (1, 0)])
    qa_line = spread(qa, X)
    g = call(join_grad, [sds((TOK, DV))] * 4, 2, ())(idx, keep, recv)
    g_line = spread(g, X)
    kv = call(
        pack_pair, [sds((TOK, DK + DV))] * 4, 2, [vm((NH, TOK, DK + DV), B16)]
    )(idx, key, value)
    res = call(
        query_part,
        [sds((TOK, NH, DK)), sds((NH, TOK, DK), F32)] + [sds((TOK + 16, DK + DV))] * 4,
        13,
        [vm((NH, TOK, DK), F32)],
    )(idx, *qa, *g, *kv, checkpoints)
    dq, qdq, kv = res[0], res[1], res[2:]
    res = call(
        line_state,
        [sds((TOK + 8, DK), F32)] * 4
        + [sds((4 * TOK, 2 * DK)), sds((4 * TOK, DV))],
        8,
        [vm((DV, DK), F32), vm((4 * TOK, DK), F32)],
        (qdq,),
    )(idx, *qa_line, *g_line)
    chunks, qa_rows, g_rows = res[:4], res[4], res[5]
    z_in = spread(chunks, Z)
    kv_line = spread(kv, X)
    total, suffix = call(
        scan_z,
        [sds((TOK + 8, DK), F32), sds((4, TOK + 8, DK), F32)],
        4,
        [vm((4, TOK + 8, DK), F32)],
    )(idx, *z_in)
    y_in = spread([total] * 4, Y)
    *carry, token = call(
        scan_y, [sds((TOK, DK), F32)] * 4 + [sds((8, 128), F32)], 5, [vm((4, TOK + 8, DK), F32)]
    )(idx, *y_in, suffix)
    carry_in = spread(carry, Z)
    near = call(
        near_part,
        [
            sds((4 * TOK, DK), F32),
            sds((4 * TOK, DV), F32),
            sds((4 * TOK, 2 * DK)),
            sds((4 * TOK, DK), F32),
            sds((4 * TOK, DV)),
            sds((4 * TOK, DK)),
        ],
        6,
        [vm((4 * TOK, DK), F32)] * 2,
        (token,),
    )(idx, qa_rows, g_rows, *kv_line)
    res = call(
        far_part,
        [sds((TOK + GROUPS, DK + DV))] * 4 + [sds((64, 2, 128), F32)],
        14,
        [vm((DV, DK), F32), vm((4, TOK + GROUPS, DK + DV), B16), vm((4, DK), F32)],
    )(idx, *carry_in, *kv_line, *near)
    back, sums = res[:4], res[4]
    back_in = spread(back, X)
    sums = lax.all_to_all(sums, SEQ, split_axis=0, concat_axis=0, tiled=True)
    dk, dv, da_part = call(
        final_part,
        [sds((TOK, NH, DK)), sds((TOK, NH, DV)), sds((TOK, NH, DK), F32)],
        6,
        [
            vm((NH, TOK, DK), B16),
            vm((NH, TOK, DV), B16),
            vm((NH, TOK, DK), B16),
            vm((NH, TOK, DK), F32),
        ],
    )(idx, *back_in, qdq, key)
    da = call(decay_part, sds((TOK, NH, DK)), 2, ())(idx, da_part, sums)
    return dq, dk, dv, da


def solution(mesh):
    torus = Mesh(mesh.devices.reshape(4, 4, 4, 2), (Y, Z, X, H))
    by_token = P(SEQ, H, None)
    placed = (
        by_token,
        by_token,
        by_token,
        P(SEQ + (H,), None, None),
        by_token,
        P(SEQ, H, None, None),
    )
    return jax.shard_map(
        whole, mesh=torus, in_specs=placed, out_specs=(by_token,) * 4, check_vma=False
    )
```

```python
import jax
import jax.numpy as jnp
from jax import lax
from jax.experimental import pallas as pl
from jax.experimental.pallas import tpu as pltpu
from jax.sharding import Mesh
from jax.sharding import PartitionSpec as P


Y, Z, X, H = "seq_0", "seq_1", "seq_2", "head"
SEQ = (Y, Z, X)
F32 = jnp.float32
B16 = jnp.bfloat16
NN = ((1,), (0,))
NT = ((1,), (1,))
TN = ((0,), (0,))
TOK, NH, DK, DV = 128, 4, 256, 512
GROUPS = 16
SCALE = DK ** (-0.5)


def split(x):
    high = x.astype(B16)
    return high, (x - high.astype(F32)).astype(B16)


def three(x):
    first = x.astype(B16)
    rest = x - first.astype(F32)
    second = rest.astype(B16)
    return first, second, (rest - second.astype(F32)).astype(B16)


def dot(a, b, dims):
    return lax.dot_general(a, b, (dims, ((), ())), preferred_element_type=F32)


def dot2(a, b, dims):
    high, low = split(a)
    return dot(high, b, dims) + dot(low, b, dims)


def dot3(a, b, dims):
    a_high, a_low = split(a)
    b_high, b_low = split(b)
    return dot(a_high, b_high, dims) + (dot(a_low, b_high, dims) + dot(a_high, b_low, dims))


def triangle(upper):
    row = lax.broadcasted_iota(jnp.int32, (TOK, TOK), 0)
    col = lax.broadcasted_iota(jnp.int32, (TOK, TOK), 1)
    return (col >= row) if upper else (col <= row)


def sds(shape, dtype=B16):
    return jax.ShapeDtypeStruct(shape, dtype)


def call(body, outs, n_in, scratch=(), after=()):
    specs = [pl.BlockSpec(memory_space=pltpu.SMEM)]
    specs += [pl.BlockSpec(memory_space=pltpu.VMEM)] * n_in
    specs += [pl.BlockSpec(memory_space=pl.ANY)] * len(after)

    def ordered(*refs):
        return body(*refs[: 1 + n_in], *refs[1 + n_in + len(after) :])

    run = pl.pallas_call(
        ordered,
        out_shape=outs,
        in_specs=specs,
        scratch_shapes=list(scratch),
        compiler_params=pltpu.CompilerParams(vmem_limit_bytes=16 * 1024 * 1024),
    )
    return lambda *operands: run(*operands, *after)


def pack_first(idx, grad, query, decay, *refs):
    outs, send, keep = refs[0:4], refs[4], refs[5]
    g, q, a, heads, scr, sems = refs[6:12]
    quarter = TOK // 4
    pieces = [pl.ds(quarter * i, quarter) for i in range(2)]
    copies = [pltpu.make_async_copy(grad.at[p], g.at[p], sems.at[i]) for i, p in enumerate(pieces)]
    copies.append(pltpu.make_async_copy(query, q, sems.at[2]))
    copies.append(pltpu.make_async_copy(decay, a, sems.at[3]))
    for copy in copies:
        copy.start()
    x, c = idx[0], idx[3]
    for i, p in enumerate(pieces):
        copies[i].wait()
        heads[:, p, :] = jnp.swapaxes(g[p], 0, 1)
    for i in range(NH):
        send[i] = heads[NH * (1 - c) + i]
        keep[i] = heads[NH * c + i]
    copies[2].wait()
    scr[:, :, :DK] = jnp.swapaxes(q[...], 0, 1)
    copies[3].wait()
    scr[:, :, DK:] = jnp.swapaxes(a[...], 0, 1)
    for s in range(4):
        outs[s][...] = scr[(x + s) % 4]


def pack_rows(a, b, out):
    width = a.shape[-1]
    out[:, :, :width] = jnp.swapaxes(a[...], 0, 1)
    out[:, :, width:] = jnp.swapaxes(b[...], 0, 1)


def pack_pair(idx, a, b, *rest):
    outs, scr = rest[:4], rest[4]
    pack_rows(a, b, scr)
    for s in range(4):
        outs[s][...] = scr[(idx[0] + s) % 4]


def join_grad(idx, keep, recv, *outs):
    c = idx[3]
    half = TOK // 2
    mine = pl.ds(pl.multiple_of(half * c, half), half)
    theirs = pl.ds(pl.multiple_of(half * (1 - c), half), half)
    for s in range(4):
        h = (idx[0] + s) % 4
        outs[s][mine, :] = keep[h]
        outs[s][theirs, :] = recv[h]


def query_part(idx, *refs):
    qa, gr, kv = refs[0:4], refs[4:8], refs[8:12]
    check = refs[12]
    dq_out, qdq_out = refs[13:15]
    kv_out = refs[15:19]
    scr = refs[19]
    low = triangle(False)
    tri = low.astype(B16)
    for s in range(4):
        h = (idx[0] + s) % 4
        q = qa[s][:, :DK].astype(F32)
        cum = dot(tri, qa[s][:, DK:], NN)
        k = kv[s][:, :DK].astype(F32)
        g = gr[s][...]
        scores = jnp.where(low, dot(g, kv[s][:, DK:], NT), 0.0)
        reached = dot(g, check[0, h], NT) + dot3(scores, k * jnp.exp(-cum), NN)
        dq = SCALE * jnp.exp(cum) * reached
        scr[h] = dq
        qdq = q * dq
        qdq_out[h] = qdq
        total = jnp.sum(qdq, axis=0, keepdims=True)
        kv_out[s][:TOK, :] = kv[s][...]
        for i, word in enumerate(three(total)):
            kv_out[s][TOK:, DK * i : DK * (i + 1)] = jnp.broadcast_to(word, (16, DK))
    dq_out[...] = jnp.swapaxes(scr[...].astype(B16), 0, 1)


def line_prep(idx, *refs):
    qa = refs[0:4]
    rise, cum, logs = refs[4:7]
    rows_qa = refs[7]
    x = idx[0]
    for s in range(4):
        j = (x - s + 4) % 4
        rows_qa[pl.ds(pl.multiple_of(TOK * j, TOK), TOK), :] = qa[s][...]
    tri = triangle(False).astype(B16)
    base = jnp.zeros((1, DK), F32)
    for j in range(4):
        rows = slice(TOK * j, TOK * (j + 1))
        inside = dot(tri, rows_qa[rows, DK:], NN) + base
        base = inside[TOK - 1 :, :]
        cum[rows, :] = inside
        q = rows_qa[rows, :DK].astype(F32)
        rise[rows, :DK], rise[rows, DK:] = split(SCALE * q * jnp.exp(inside))
    logs[...] = jnp.broadcast_to(base, (8, DK))


def line_state(idx, *refs):
    gr, rise, logs = refs[0:4], refs[4], refs[5]
    chunks, g_out = refs[6:10], refs[10]
    acc = refs[11]
    x, z = idx[0], idx[1]
    for s in range(4):
        j = (x - s + 4) % 4
        g_out[pl.ds(pl.multiple_of(TOK * j, TOK), TOK), :] = gr[s][...]
    both = dot(g_out[...], rise[...], TN)
    acc[...] = both[:, :DK] + both[:, DK:]
    for s in range(4):
        at = pl.multiple_of(TOK * ((z + s) % 4), TOK)
        chunks[s][:TOK, :] = acc[pl.ds(at, TOK), :]
        chunks[s][TOK:, :] = logs[...]


def scan_z(idx, *refs):
    parts = refs[0:4]
    total, suffix = refs[4:6]
    scr = refs[6]
    z = idx[1]
    for s in range(4):
        scr[(z - s + 4) % 4] = parts[s][...]
    state = jnp.zeros((TOK, DK), F32)
    logs = jnp.zeros((1, DK), F32)
    for j in reversed(range(4)):
        suffix[j, :TOK, :] = state
        suffix[j, TOK:, :] = jnp.broadcast_to(logs, (8, DK))
        own = scr[j, TOK : TOK + 1, :]
        state = jnp.exp(own) * state + scr[j, :TOK, :]
        logs = logs + own
    total[:TOK, :] = state
    total[TOK:, :] = jnp.broadcast_to(logs, (8, DK))


def scan_y(idx, *refs):
    parts, suffix = refs[0:4], refs[4]
    outs, token = refs[5:9], refs[9]
    scr = refs[10]
    y, z = idx[2], idx[1]
    token[...] = jnp.zeros((8, 128), F32)
    for s in range(4):
        scr[(y - s + 4) % 4] = parts[s][...]
    state = jnp.zeros((TOK, DK), F32)
    for j in (3, 2, 1):
        joined = jnp.exp(scr[j, TOK : TOK + 1, :]) * state + scr[j, :TOK, :]
        state = jnp.where(j > y, joined, state)
    for s in range(4):
        j = (z + s) % 4
        outs[s][...] = suffix[j, :TOK, :] + jnp.exp(suffix[j, TOK : TOK + 1, :]) * state


def near_part(idx, *refs):
    g, rise, cum = refs[0:3]
    kv = refs[3:7]
    dk_near, dv_near, k_end, ends, v_out, k_out = refs[7:13]
    x = idx[0]
    for s in range(4):
        j = (x - s + 4) % 4
        rows = pl.ds(pl.multiple_of(TOK * j, TOK), TOK)
        k_out[rows, :] = kv[s][:TOK, :DK]
        v_out[rows, :] = kv[s][:TOK, DK:]
    end = jnp.exp(cum[4 * TOK - 1 :, :] - cum[...])
    ends[...] = end
    k_high, k_low = split(k_out[...].astype(F32) * end)
    k_end[:, :DK] = k_high
    k_end[:, DK : 2 * DK] = k_low
    k_end[:, 2 * DK :] = k_high
    for j in range(4):
        rows = slice(TOK * j, TOK * (j + 1))
        width = 4 * TOK - TOK * j
        later = slice(TOK * j, 4 * TOK)
        fall = jnp.exp(-cum[rows, :])
        keep = lax.broadcasted_iota(jnp.int32, (TOK, width), 1) >= lax.broadcasted_iota(
            jnp.int32, (TOK, width), 0
        )
        high, lo = rise[later, :DK], rise[later, DK:]
        scores = jnp.where(keep, dot(v_out[rows, :], g[later, :], NT), 0.0)
        s_high, s_low = split(scores)
        dk_near[rows, :] = fall * (
            dot(s_high, high, NN) + (dot(s_low, high, NN) + dot(s_high, lo, NN))
        )
        f_high, f_low = split(k_out[rows, :].astype(F32) * fall)
        affinity = dot(f_high, high, NT) + (dot(f_low, high, NT) + dot(f_high, lo, NT))
        dv_near[rows, :] = dot2(jnp.where(keep, affinity, 0.0), g[later, :], NN)


def far_part(idx, *refs):
    parts = refs[0:4]
    kv = refs[4:8]
    dk_near, dv_near, k_end, ends, v, k = refs[8:14]
    outs = refs[14:18]
    sums = refs[18]
    state, dk_all, dv_all, ahead, total = refs[19:24]
    x, z = idx[0], idx[1]
    for s in range(4):
        j = (z - s + 4) % 4
        rows = pl.ds(pl.multiple_of(TOK * j, TOK), TOK)
        high, lo = split(parts[s][...])
        state[rows, :DK] = high
        state[rows, DK : 2 * DK] = high
        state[rows, 2 * DK :] = lo
    reached = dot(v[...], state[:, :DK], NN) + dot(v[...], state[:, 2 * DK :], NN)
    dk = dk_near[...] + ends[...] * reached
    dk_all[...] = dk
    dv_all[...] = dv_near[...] + dot(k_end[...], state[...], NT)
    kdk_high, kdk_low = split(k[...].astype(F32) * dk)
    group = lax.broadcasted_iota(jnp.int32, (4 * GROUPS + 8, 4 * TOK), 0)
    token = lax.broadcasted_iota(jnp.int32, (4 * GROUPS + 8, 4 * TOK), 1)
    first = jnp.where(group < 4 * GROUPS, (group + 1) * (TOK // GROUPS), 0)
    after = (token >= first).astype(B16)
    behind = dot(after, kdk_high, NN) + dot(after, kdk_low, NN)
    for s in range(4):
        j = (x - s + 4) % 4
        total[pl.ds(j, 1), :] = (
            kv[s][TOK : TOK + 1, :DK].astype(F32)
            + kv[s][TOK : TOK + 1, DK : 2 * DK].astype(F32)
            + kv[s][TOK : TOK + 1, 2 * DK :].astype(F32)
        )
    running = jnp.zeros((1, DK), F32)
    for j in reversed(range(4)):
        rows = slice(GROUPS * j, GROUPS * (j + 1))
        for i, word in enumerate(three(running - behind[rows, :])):
            ahead[j, :, DK * i : DK * (i + 1)] = word
        running = running + total[j : j + 1, :]
    running = running - behind[4 * GROUPS : 4 * GROUPS + 1, :]
    block = jnp.concatenate([running[:, :128], running[:, 128:]], axis=0)
    for d in range(64):
        sums[d] = block
    for s in range(4):
        j = (x + s) % 4
        rows = pl.ds(pl.multiple_of(TOK * j, TOK), TOK)
        outs[s][:TOK, :DK] = dk_all[rows, :].astype(B16)
        outs[s][:TOK, DK:] = dv_all[rows, :].astype(B16)
        outs[s][TOK:, :] = ahead[j]


def final_part(idx, *refs):
    parts = refs[0:4]
    qdq, key = refs[4:6]
    dk_out, dv_out, da_part = refs[6:9]
    s_dk, s_dv, s_k, s_da = refs[9:13]
    x = idx[0]
    s_k[...] = jnp.swapaxes(key[...], 0, 1)
    row = lax.broadcasted_iota(jnp.int32, (TOK, TOK), 0)
    col = lax.broadcasted_iota(jnp.int32, (TOK, TOK), 1)
    size = TOK // GROUPS
    upper = (col >= row).astype(B16)
    inner = ((col >= row) & (col // size == row // size)).astype(B16)
    pick_row = lax.broadcasted_iota(jnp.int32, (TOK, GROUPS), 0)
    pick_col = lax.broadcasted_iota(jnp.int32, (TOK, GROUPS), 1)
    pick = (pick_row // size == pick_col).astype(B16)
    for s in range(4):
        h = (x - s + 4) % 4
        dk = parts[s][:TOK, :DK]
        s_dk[h] = dk
        s_dv[h] = parts[s][:TOK, DK:]
        q_high, q_low = split(qdq[h])
        k_high, k_low = split(s_k[h].astype(F32) * dk.astype(F32))
        ahead = (
            dot(pick, parts[s][TOK:, :DK], NN)
            + dot(pick, parts[s][TOK:, DK : 2 * DK], NN)
            + dot(pick, parts[s][TOK:, 2 * DK :], NN)
        )
        s_da[h] = (
            (dot(upper, q_high, NN) + dot(upper, q_low, NN))
            - (dot(inner, k_high, NN) + dot(inner, k_low, NN))
            + ahead
        )
    dk_out[...] = jnp.swapaxes(s_dk[...], 0, 1)
    dv_out[...] = jnp.swapaxes(s_dv[...], 0, 1)
    da_part[...] = jnp.swapaxes(s_da[...], 0, 1)


def decay_part(idx, da_part, sums, da_out, rounded, sems):
    line = idx[2] * 4 + idx[1]
    later = []
    for h in range(NH):
        acc = jnp.zeros((2, 128), F32)
        for l in range(1, 16):
            acc = acc + jnp.where(l > line, sums[4 * l + h], 0.0)
        later.append(jnp.concatenate([acc[0:1], acc[1:2]], axis=1))
    later = jnp.concatenate(later, axis=0)[None]
    copies = []
    for i in range(2):
        rows = pl.ds(TOK // 2 * i, TOK // 2)
        rounded[rows] = (da_part[rows] + later).astype(B16)
        copies.append(pltpu.make_async_copy(rounded.at[rows], da_out.at[rows], sems.at[i]))
        copies[i].start()
    for copy in copies:
        copy.wait()


def shifted(value, axis, s):
    return lax.ppermute(value, axis, [(i, (i + s) % 4) for i in range(4)])


def spread(parts, axis):
    moved = [parts[0]]
    for s in (1, 2, 3):
        moved.append(shifted(parts[s], axis, s))
    return moved


def whole(query, key, value, out_grad, log_decay, checkpoints):
    x, z, y, c = (lax.axis_index(axis) for axis in (X, Z, Y, H))
    idx = jnp.stack([x, z, y, c]).astype(jnp.int32)
    vm = pltpu.VMEM

    half = TOK // 2
    hbm = pl.BlockSpec(memory_space=pltpu.HBM)
    *qa, send, keep = pl.pallas_call(
        pack_first,
        out_shape=[sds((TOK, 2 * DK))] * 4 + [sds((NH, half, DV))] * 2,
        in_specs=[pl.BlockSpec(memory_space=pltpu.SMEM), hbm, hbm, hbm],
        scratch_shapes=[
            vm((half, 2 * NH, DV), B16),
            vm((TOK, NH, DK), B16),
            vm((TOK, NH, DK), B16),
            vm((2 * NH, half, DV), B16),
            vm((NH, TOK, 2 * DK), B16),
            pltpu.SemaphoreType.DMA((4,)),
        ],
        name="pack_first",
        compiler_params=pltpu.CompilerParams(vmem_limit_bytes=16 * 1024 * 1024),
    )(idx, *(pltpu.with_memory_space_constraint(a, pltpu.HBM) for a in (out_grad, query, log_decay)))
    recv = lax.ppermute(send, H, [(0, 1), (1, 0)])
    qa_line = spread(qa, X)
    g = call(join_grad, [sds((TOK, DV))] * 4, 2, ())(idx, keep, recv)
    g_line = spread(g, X)
    kv = call(
        pack_pair, [sds((TOK, DK + DV))] * 4, 2, [vm((NH, TOK, DK + DV), B16)]
    )(idx, key, value)
    res = call(
        query_part,
        [sds((TOK, NH, DK)), sds((NH, TOK, DK), F32)] + [sds((TOK + 16, DK + DV))] * 4,
        13,
        [vm((NH, TOK, DK), F32)],
    )(idx, *qa, *g, *kv, checkpoints)
    dq, qdq, kv = res[0], res[1], res[2:]
    rise, cum, logs = call(
        line_prep,
        [sds((4 * TOK, 2 * DK)), sds((4 * TOK, DK), F32), sds((8, DK), F32)],
        4,
        [vm((4 * TOK, 2 * DK), B16)],
    )(idx, *qa_line)
    *chunks, g_rows = call(
        line_state,
        [sds((TOK + 8, DK), F32)] * 4 + [sds((4 * TOK, DV))],
        6,
        [vm((DV, DK), F32)],
        (qdq,),
    )(idx, *g_line, rise, logs)
    z_in = spread(chunks, Z)
    kv_line = spread(kv, X)
    total, suffix = call(
        scan_z,
        [sds((TOK + 8, DK), F32), sds((4, TOK + 8, DK), F32)],
        4,
        [vm((4, TOK + 8, DK), F32)],
    )(idx, *z_in)
    y_in = spread([total] * 4, Y)
    *carry, token = call(
        scan_y, [sds((TOK, DK), F32)] * 4 + [sds((8, 128), F32)], 5, [vm((4, TOK + 8, DK), F32)]
    )(idx, *y_in, suffix)
    carry_in = spread(carry, Z)
    near = call(
        near_part,
        [
            sds((4 * TOK, DK), F32),
            sds((4 * TOK, DV), F32),
            sds((4 * TOK, 3 * DK)),
            sds((4 * TOK, DK), F32),
            sds((4 * TOK, DV)),
            sds((4 * TOK, DK)),
        ],
        7,
        (),
        (token,),
    )(idx, g_rows, rise, cum, *kv_line)
    res = call(
        far_part,
        [sds((TOK + GROUPS, DK + DV))] * 4 + [sds((64, 2, 128), F32)],
        14,
        [
            vm((DV, 3 * DK), B16),
            vm((4 * TOK, DK), F32),
            vm((4 * TOK, DV), F32),
            vm((4, GROUPS, DK + DV), B16),
            vm((4, DK), F32),
        ],
    )(idx, *carry_in, *kv_line, *near)
    back, sums = res[:4], res[4]
    back_in = spread(back, X)
    sums = lax.all_to_all(sums, SEQ, split_axis=0, concat_axis=0, tiled=True)
    dk, dv, da_part = call(
        final_part,
        [sds((TOK, NH, DK)), sds((TOK, NH, DV)), sds((TOK, NH, DK), F32)],
        6,
        [
            vm((NH, TOK, DK), B16),
            vm((NH, TOK, DV), B16),
            vm((NH, TOK, DK), B16),
            vm((NH, TOK, DK), F32),
        ],
    )(idx, *back_in, qdq, key)
    vmem = pl.BlockSpec(memory_space=pltpu.VMEM)
    da = pl.pallas_call(
        decay_part,
        out_shape=sds((TOK, NH, DK)),
        in_specs=[pl.BlockSpec(memory_space=pltpu.SMEM), vmem, vmem],
        out_specs=hbm,
        scratch_shapes=[vm((TOK, NH, DK), B16), pltpu.SemaphoreType.DMA((2,))],
        name="decay_part",
        compiler_params=pltpu.CompilerParams(vmem_limit_bytes=16 * 1024 * 1024),
    )(idx, da_part, sums)
    return dq, dk, dv, da


def solution(mesh):
    torus = Mesh(mesh.devices.reshape(4, 4, 4, 2), (Y, Z, X, H))
    by_token = P(SEQ, H, None)
    placed = (
        by_token,
        by_token,
        by_token,
        P(SEQ + (H,), None, None),
        by_token,
        P(SEQ, H, None, None),
    )
    return jax.shard_map(
        whole, mesh=torus, in_specs=placed, out_specs=(by_token,) * 4, check_vma=False
    )
```

```python
import jax
import jax.numpy as jnp
from jax import lax
from jax.experimental import pallas as pl
from jax.experimental.pallas import tpu as pltpu
from jax.sharding import Mesh
from jax.sharding import PartitionSpec as P


Y, Z, X, H = "seq_0", "seq_1", "seq_2", "head"
SEQ = (Y, Z, X)
F32 = jnp.float32
B16 = jnp.bfloat16
NN = ((1,), (0,))
NT = ((1,), (1,))
TN = ((0,), (0,))
TOK, NH, DK, DV = 128, 4, 256, 512
GROUPS = 16
SCALE = DK ** (-0.5)


def split(x):
    high = x.astype(B16)
    return high, (x - high.astype(F32)).astype(B16)


def three(x):
    first = x.astype(B16)
    rest = x - first.astype(F32)
    second = rest.astype(B16)
    return first, second, (rest - second.astype(F32)).astype(B16)


def dot(a, b, dims):
    return lax.dot_general(a, b, (dims, ((), ())), preferred_element_type=F32)


def dot2(a, b, dims):
    high, low = split(a)
    return dot(high, b, dims) + dot(low, b, dims)


def dot3(a, b, dims):
    a_high, a_low = split(a)
    b_high, b_low = split(b)
    return dot(a_high, b_high, dims) + (dot(a_low, b_high, dims) + dot(a_high, b_low, dims))


def triangle(upper):
    row = lax.broadcasted_iota(jnp.int32, (TOK, TOK), 0)
    col = lax.broadcasted_iota(jnp.int32, (TOK, TOK), 1)
    return (col >= row) if upper else (col <= row)


def sds(shape, dtype=B16):
    return jax.ShapeDtypeStruct(shape, dtype)


def placed_kernel(body):
    def run(*refs):
        return body(tuple(lax.axis_index(axis) for axis in (X, Z, Y, H)), *refs)

    return run


def call(body, outs, n_in, scratch=(), after=()):
    specs = [pl.BlockSpec(memory_space=pltpu.VMEM)] * n_in
    specs += [pl.BlockSpec(memory_space=pl.ANY)] * len(after)

    def ordered(idx, *refs):
        return body(idx, *refs[:n_in], *refs[n_in + len(after) :])

    run = pl.pallas_call(
        placed_kernel(ordered),
        out_shape=outs,
        in_specs=specs,
        scratch_shapes=list(scratch),
        compiler_params=pltpu.CompilerParams(vmem_limit_bytes=16 * 1024 * 1024),
    )
    return lambda *operands: run(*operands, *after)


def pack_first(idx, grad, query, decay, *refs):
    outs, send, keep = refs[0:4], refs[4], refs[5]
    g, q, a, heads, scr, sems = refs[6:12]
    quarter = TOK // 4
    pieces = [pl.ds(quarter * i, quarter) for i in range(2)]
    copies = [pltpu.make_async_copy(grad.at[p], g.at[p], sems.at[i]) for i, p in enumerate(pieces)]
    copies.append(pltpu.make_async_copy(query, q, sems.at[2]))
    copies.append(pltpu.make_async_copy(decay, a, sems.at[3]))
    for copy in copies:
        copy.start()
    x, c = idx[0], idx[3]
    for i, p in enumerate(pieces):
        copies[i].wait()
        heads[:, p, :] = jnp.swapaxes(g[p], 0, 1)
    for i in range(NH):
        send[i] = heads[NH * (1 - c) + i]
        keep[i] = heads[NH * c + i]
    copies[2].wait()
    scr[:, :, :DK] = jnp.swapaxes(q[...], 0, 1)
    copies[3].wait()
    scr[:, :, DK:] = jnp.swapaxes(a[...], 0, 1)
    for s in range(4):
        outs[s][...] = scr[(x + s) % 4]


def pack_rows(a, b, out):
    width = a.shape[-1]
    out[:, :, :width] = jnp.swapaxes(a[...], 0, 1)
    out[:, :, width:] = jnp.swapaxes(b[...], 0, 1)


def pack_pair(idx, a, b, *rest):
    outs, scr = rest[:4], rest[4]
    pack_rows(a, b, scr)
    for s in range(4):
        outs[s][...] = scr[(idx[0] + s) % 4]


def join_grad(idx, keep, recv, *outs):
    c = idx[3]
    half = TOK // 2
    mine = pl.ds(pl.multiple_of(half * c, half), half)
    theirs = pl.ds(pl.multiple_of(half * (1 - c), half), half)
    for s in range(4):
        h = (idx[0] + s) % 4
        outs[s][mine, :] = keep[h]
        outs[s][theirs, :] = recv[h]


def query_part(idx, *refs):
    qa, gr, kv = refs[0:4], refs[4:8], refs[8:12]
    check = refs[12]
    dq_out, qdq_out = refs[13:15]
    kv_out = refs[15:19]
    scr = refs[19]
    low = triangle(False)
    tri = low.astype(B16)
    for s in range(4):
        h = (idx[0] + s) % 4
        q = qa[s][:, :DK].astype(F32)
        cum = dot(tri, qa[s][:, DK:], NN)
        k = kv[s][:, :DK].astype(F32)
        g = gr[s][...]
        scores = jnp.where(low, dot(g, kv[s][:, DK:], NT), 0.0)
        reached = dot(g, check[0, h], NT) + dot3(scores, k * jnp.exp(-cum), NN)
        dq = SCALE * jnp.exp(cum) * reached
        scr[h] = dq
        qdq = q * dq
        qdq_out[h] = qdq
        total = jnp.sum(qdq, axis=0, keepdims=True)
        kv_out[s][:TOK, :] = kv[s][...]
        for i, word in enumerate(three(total)):
            kv_out[s][TOK:, DK * i : DK * (i + 1)] = jnp.broadcast_to(word, (16, DK))
    dq_out[...] = jnp.swapaxes(scr[...].astype(B16), 0, 1)


def line_prep(idx, *refs):
    qa = refs[0:4]
    rise, cum, logs = refs[4:7]
    rows_qa = refs[7]
    x = idx[0]
    for s in range(4):
        j = (x - s + 4) % 4
        rows_qa[pl.ds(pl.multiple_of(TOK * j, TOK), TOK), :] = qa[s][...]
    tri = triangle(False).astype(B16)
    base = jnp.zeros((1, DK), F32)
    for j in range(4):
        rows = slice(TOK * j, TOK * (j + 1))
        inside = dot(tri, rows_qa[rows, DK:], NN) + base
        base = inside[TOK - 1 :, :]
        cum[rows, :] = inside
        q = rows_qa[rows, :DK].astype(F32)
        rise[rows, :DK], rise[rows, DK:] = split(SCALE * q * jnp.exp(inside))
    logs[...] = jnp.broadcast_to(base, (8, DK))


def line_state(idx, *refs):
    gr, rise, logs = refs[0:4], refs[4], refs[5]
    chunks, g_out = refs[6:10], refs[10]
    acc = refs[11]
    x, z = idx[0], idx[1]
    for s in range(4):
        j = (x - s + 4) % 4
        g_out[pl.ds(pl.multiple_of(TOK * j, TOK), TOK), :] = gr[s][...]
    both = dot(g_out[...], rise[...], TN)
    acc[...] = both[:, :DK] + both[:, DK:]
    for s in range(4):
        at = pl.multiple_of(TOK * ((z + s) % 4), TOK)
        chunks[s][:TOK, :] = acc[pl.ds(at, TOK), :]
        chunks[s][TOK:, :] = logs[...]


def scan_z(idx, *refs):
    parts = refs[0:4]
    total, suffix = refs[4:6]
    scr = refs[6]
    z = idx[1]
    for s in range(4):
        scr[(z - s + 4) % 4] = parts[s][...]
    state = jnp.zeros((TOK, DK), F32)
    logs = jnp.zeros((1, DK), F32)
    for j in reversed(range(4)):
        suffix[j, :TOK, :] = state
        suffix[j, TOK:, :] = jnp.broadcast_to(logs, (8, DK))
        own = scr[j, TOK : TOK + 1, :]
        state = jnp.exp(own) * state + scr[j, :TOK, :]
        logs = logs + own
    total[:TOK, :] = state
    total[TOK:, :] = jnp.broadcast_to(logs, (8, DK))


def scan_y(idx, *refs):
    parts, suffix = refs[0:4], refs[4]
    outs, token = refs[5:9], refs[9]
    scr = refs[10]
    y, z = idx[2], idx[1]
    token[...] = jnp.zeros((8, 128), F32)
    for s in range(4):
        scr[(y - s + 4) % 4] = parts[s][...]
    state = jnp.zeros((TOK, DK), F32)
    for j in (3, 2, 1):
        joined = jnp.exp(scr[j, TOK : TOK + 1, :]) * state + scr[j, :TOK, :]
        state = jnp.where(j > y, joined, state)
    for s in range(4):
        j = (z + s) % 4
        outs[s][...] = suffix[j, :TOK, :] + jnp.exp(suffix[j, TOK : TOK + 1, :]) * state


def near_part(idx, *refs):
    g, rise, cum = refs[0:3]
    kv = refs[3:7]
    dk_near, dv_near, k_end, ends, v_out, k_out = refs[7:13]
    x = idx[0]
    for s in range(4):
        j = (x - s + 4) % 4
        rows = pl.ds(pl.multiple_of(TOK * j, TOK), TOK)
        k_out[rows, :] = kv[s][:TOK, :DK]
        v_out[rows, :] = kv[s][:TOK, DK:]
    end = jnp.exp(cum[4 * TOK - 1 :, :] - cum[...])
    ends[...] = end
    k_high, k_low = split(k_out[...].astype(F32) * end)
    k_end[:, :DK] = k_high
    k_end[:, DK : 2 * DK] = k_low
    k_end[:, 2 * DK :] = k_high
    for j in range(4):
        rows = slice(TOK * j, TOK * (j + 1))
        width = 4 * TOK - TOK * j
        later = slice(TOK * j, 4 * TOK)
        fall = jnp.exp(-cum[rows, :])
        keep = lax.broadcasted_iota(jnp.int32, (TOK, width), 1) >= lax.broadcasted_iota(
            jnp.int32, (TOK, width), 0
        )
        high, lo = rise[later, :DK], rise[later, DK:]
        scores = jnp.where(keep, dot(v_out[rows, :], g[later, :], NT), 0.0)
        s_high, s_low = split(scores)
        dk_near[rows, :] = fall * (
            dot(s_high, high, NN) + (dot(s_low, high, NN) + dot(s_high, lo, NN))
        )
        f_high, f_low = split(k_out[rows, :].astype(F32) * fall)
        affinity = dot(f_high, high, NT) + (dot(f_low, high, NT) + dot(f_high, lo, NT))
        dv_near[rows, :] = dot2(jnp.where(keep, affinity, 0.0), g[later, :], NN)


def far_part(idx, *refs):
    parts = refs[0:4]
    kv = refs[4:8]
    dk_near, dv_near, k_end, ends, v, k = refs[8:14]
    outs = refs[14:18]
    sums = refs[18]
    state, dk_all, dv_all, ahead, total = refs[19:24]
    x, z = idx[0], idx[1]
    for s in range(4):
        j = (z - s + 4) % 4
        rows = pl.ds(pl.multiple_of(TOK * j, TOK), TOK)
        high, lo = split(parts[s][...])
        state[rows, :DK] = high
        state[rows, DK : 2 * DK] = high
        state[rows, 2 * DK :] = lo
    reached = dot(v[...], state[:, :DK], NN) + dot(v[...], state[:, 2 * DK :], NN)
    dk = dk_near[...] + ends[...] * reached
    dk_all[...] = dk
    dv_all[...] = dv_near[...] + dot(k_end[...], state[...], NT)
    kdk_high, kdk_low = split(k[...].astype(F32) * dk)
    group = lax.broadcasted_iota(jnp.int32, (4 * GROUPS + 8, 4 * TOK), 0)
    token = lax.broadcasted_iota(jnp.int32, (4 * GROUPS + 8, 4 * TOK), 1)
    first = jnp.where(group < 4 * GROUPS, (group + 1) * (TOK // GROUPS), 0)
    after = (token >= first).astype(B16)
    behind = dot(after, kdk_high, NN) + dot(after, kdk_low, NN)
    for s in range(4):
        j = (x - s + 4) % 4
        total[pl.ds(j, 1), :] = (
            kv[s][TOK : TOK + 1, :DK].astype(F32)
            + kv[s][TOK : TOK + 1, DK : 2 * DK].astype(F32)
            + kv[s][TOK : TOK + 1, 2 * DK :].astype(F32)
        )
    running = jnp.zeros((1, DK), F32)
    for j in reversed(range(4)):
        rows = slice(GROUPS * j, GROUPS * (j + 1))
        for i, word in enumerate(three(running - behind[rows, :])):
            ahead[j, :, DK * i : DK * (i + 1)] = word
        running = running + total[j : j + 1, :]
    running = running - behind[4 * GROUPS : 4 * GROUPS + 1, :]
    block = jnp.concatenate([running[:, :128], running[:, 128:]], axis=0)
    for d in range(64):
        sums[d] = block
    for s in range(4):
        j = (x + s) % 4
        rows = pl.ds(pl.multiple_of(TOK * j, TOK), TOK)
        outs[s][:TOK, :DK] = dk_all[rows, :].astype(B16)
        outs[s][:TOK, DK:] = dv_all[rows, :].astype(B16)
        outs[s][TOK:, :] = ahead[j]


def final_part(idx, *refs):
    parts = refs[0:4]
    qdq, key = refs[4:6]
    dk_out, dv_out, da_part = refs[6:9]
    s_dk, s_dv, s_k, s_da = refs[9:13]
    x = idx[0]
    s_k[...] = jnp.swapaxes(key[...], 0, 1)
    row = lax.broadcasted_iota(jnp.int32, (TOK, TOK), 0)
    col = lax.broadcasted_iota(jnp.int32, (TOK, TOK), 1)
    size = TOK // GROUPS
    upper = (col >= row).astype(B16)
    inner = ((col >= row) & (col // size == row // size)).astype(B16)
    pick_row = lax.broadcasted_iota(jnp.int32, (TOK, GROUPS), 0)
    pick_col = lax.broadcasted_iota(jnp.int32, (TOK, GROUPS), 1)
    pick = (pick_row // size == pick_col).astype(B16)
    for s in range(4):
        h = (x - s + 4) % 4
        dk = parts[s][:TOK, :DK]
        s_dk[h] = dk
        s_dv[h] = parts[s][:TOK, DK:]
        q_high, q_low = split(qdq[h])
        k_high, k_low = split(s_k[h].astype(F32) * dk.astype(F32))
        ahead = (
            dot(pick, parts[s][TOK:, :DK], NN)
            + dot(pick, parts[s][TOK:, DK : 2 * DK], NN)
            + dot(pick, parts[s][TOK:, 2 * DK :], NN)
        )
        s_da[h] = (
            (dot(upper, q_high, NN) + dot(upper, q_low, NN))
            - (dot(inner, k_high, NN) + dot(inner, k_low, NN))
            + ahead
        )
    dk_out[...] = jnp.swapaxes(s_dk[...], 0, 1)
    dv_out[...] = jnp.swapaxes(s_dv[...], 0, 1)
    da_part[...] = jnp.swapaxes(s_da[...], 0, 1)


def decay_part(idx, da_part, sums, da_out, rounded, sems):
    line = idx[2] * 4 + idx[1]
    later = []
    for h in range(NH):
        acc = jnp.zeros((2, 128), F32)
        for l in range(1, 16):
            acc = acc + jnp.where(l > line, sums[4 * l + h], 0.0)
        later.append(jnp.concatenate([acc[0:1], acc[1:2]], axis=1))
    later = jnp.concatenate(later, axis=0)[None]
    copies = []
    for i in range(2):
        rows = pl.ds(TOK // 2 * i, TOK // 2)
        rounded[rows] = (da_part[rows] + later).astype(B16)
        copies.append(pltpu.make_async_copy(rounded.at[rows], da_out.at[rows], sems.at[i]))
        copies[i].start()
    for copy in copies:
        copy.wait()


def shifted(value, axis, s):
    return lax.ppermute(value, axis, [(i, (i + s) % 4) for i in range(4)])


def spread(parts, axis):
    moved = [parts[0]]
    for s in (1, 2, 3):
        moved.append(shifted(parts[s], axis, s))
    return moved


def whole(query, key, value, out_grad, log_decay, checkpoints):
    vm = pltpu.VMEM

    half = TOK // 2
    hbm = pl.BlockSpec(memory_space=pltpu.HBM)
    *qa, send, keep = pl.pallas_call(
        placed_kernel(pack_first),
        out_shape=[sds((TOK, 2 * DK))] * 4 + [sds((NH, half, DV))] * 2,
        in_specs=[hbm, hbm, hbm],
        scratch_shapes=[
            vm((half, 2 * NH, DV), B16),
            vm((TOK, NH, DK), B16),
            vm((TOK, NH, DK), B16),
            vm((2 * NH, half, DV), B16),
            vm((NH, TOK, 2 * DK), B16),
            pltpu.SemaphoreType.DMA((4,)),
        ],
        name="pack_first",
        compiler_params=pltpu.CompilerParams(vmem_limit_bytes=16 * 1024 * 1024),
    )(*(pltpu.with_memory_space_constraint(a, pltpu.HBM) for a in (out_grad, query, log_decay)))
    recv = lax.ppermute(send, H, [(0, 1), (1, 0)])
    qa_line = spread(qa, X)
    g = call(join_grad, [sds((TOK, DV))] * 4, 2, ())(keep, recv)
    g_line = spread(g, X)
    kv = call(pack_pair, [sds((TOK, DK + DV))] * 4, 2, [vm((NH, TOK, DK + DV), B16)])(key, value)
    res = call(
        query_part,
        [sds((TOK, NH, DK)), sds((NH, TOK, DK), F32)] + [sds((TOK + 16, DK + DV))] * 4,
        13,
        [vm((NH, TOK, DK), F32)],
    )(*qa, *g, *kv, checkpoints)
    dq, qdq, kv = res[0], res[1], res[2:]
    rise, cum, logs = call(
        line_prep,
        [sds((4 * TOK, 2 * DK)), sds((4 * TOK, DK), F32), sds((8, DK), F32)],
        4,
        [vm((4 * TOK, 2 * DK), B16)],
    )(*qa_line)
    *chunks, g_rows = call(
        line_state,
        [sds((TOK + 8, DK), F32)] * 4 + [sds((4 * TOK, DV))],
        6,
        [vm((DV, DK), F32)],
        (qdq,),
    )(*g_line, rise, logs)
    z_in = spread(chunks, Z)
    kv_line = spread(kv, X)
    total, suffix = call(
        scan_z,
        [sds((TOK + 8, DK), F32), sds((4, TOK + 8, DK), F32)],
        4,
        [vm((4, TOK + 8, DK), F32)],
    )(*z_in)
    y_in = spread([total] * 4, Y)
    *carry, token = call(
        scan_y, [sds((TOK, DK), F32)] * 4 + [sds((8, 128), F32)], 5, [vm((4, TOK + 8, DK), F32)]
    )(*y_in, suffix)
    carry_in = spread(carry, Z)
    near = call(
        near_part,
        [
            sds((4 * TOK, DK), F32),
            sds((4 * TOK, DV), F32),
            sds((4 * TOK, 3 * DK)),
            sds((4 * TOK, DK), F32),
            sds((4 * TOK, DV)),
            sds((4 * TOK, DK)),
        ],
        7,
        (),
        (token,),
    )(g_rows, rise, cum, *kv_line)
    res = call(
        far_part,
        [sds((TOK + GROUPS, DK + DV))] * 4 + [sds((64, 2, 128), F32)],
        14,
        [
            vm((DV, 3 * DK), B16),
            vm((4 * TOK, DK), F32),
            vm((4 * TOK, DV), F32),
            vm((4, GROUPS, DK + DV), B16),
            vm((4, DK), F32),
        ],
    )(*carry_in, *kv_line, *near)
    back, sums = res[:4], res[4]
    back_in = spread(back, X)
    sums = lax.all_to_all(sums, SEQ, split_axis=0, concat_axis=0, tiled=True)
    dk, dv, da_part = call(
        final_part,
        [sds((TOK, NH, DK)), sds((TOK, NH, DV)), sds((TOK, NH, DK), F32)],
        6,
        [
            vm((NH, TOK, DK), B16),
            vm((NH, TOK, DV), B16),
            vm((NH, TOK, DK), B16),
            vm((NH, TOK, DK), F32),
        ],
    )(*back_in, qdq, key)
    vmem = pl.BlockSpec(memory_space=pltpu.VMEM)
    da = pl.pallas_call(
        placed_kernel(decay_part),
        out_shape=sds((TOK, NH, DK)),
        in_specs=[vmem, vmem],
        out_specs=hbm,
        scratch_shapes=[vm((TOK, NH, DK), B16), pltpu.SemaphoreType.DMA((2,))],
        name="decay_part",
        compiler_params=pltpu.CompilerParams(vmem_limit_bytes=16 * 1024 * 1024),
    )(da_part, sums)
    return dq, dk, dv, da


def solution(mesh):
    torus = Mesh(mesh.devices.reshape(4, 4, 4, 2), (Y, Z, X, H))
    by_token = P(SEQ, H, None)
    placed = (
        by_token,
        by_token,
        by_token,
        P(SEQ + (H,), None, None),
        by_token,
        P(SEQ, H, None, None),
    )
    return jax.shard_map(
        whole, mesh=torus, in_specs=placed, out_specs=(by_token,) * 4, check_vma=False
    )
```
